8 devices in a mesh: rep: 1 (over z), dp: 8 (over x, y, core).
Axes of the slice: x: 2, y: 2, z: 1, core: 2. Of those that a mesh axis runs over, the one named last changes fastest.
Arguments:
- x: bfloat16 [8, 2048, 1024], P(('rep', 'dp'))
- dy: bfloat16 [8, 2048, 1024], P(('rep', 'dp'))
- wq: bfloat16 [2, 1024, 1536], replicated
- wk: bfloat16 [2, 1024, 1536], replicated
- wv: bfloat16 [2, 1024, 1536], replicated
- wo: bfloat16 [2, 1536, 1024], replicated
- w_gate: bfloat16 [2, 1024, 4096], replicated
- w_up: bfloat16 [2, 1024, 4096], replicated
- w_down: bfloat16 [2, 4096, 1024], replicated
- m_wq: float32 [2, 1024, 1536], replicated
- m_wk: float32 [2, 1024, 1536], replicated
- m_wv: float32 [2, 1024, 1536], replicated
- m_wo: float32 [2, 1536, 1024], replicated
- m_w_gate: float32 [2, 1024, 4096], replicated
- m_w_up: float32 [2, 1024, 4096], replicated
- m_w_down: float32 [2, 4096, 1024], replicated
- v_wq: float32 [2, 1024, 1536], replicated
- v_wk: float32 [2, 1024, 1536], replicated
- v_wv: float32 [2, 1024, 1536], replicated
- v_wo: float32 [2, 1536, 1024], replicated
- v_w_gate: float32 [2, 1024, 4096], replicated
- v_w_up: float32 [2, 1024, 4096], replicated
- v_w_down: float32 [2, 4096, 1024], replicated
Outputs:
- output 1: bfloat16 [2, 1024, 1536], P('rep')
- output 2: bfloat16 [2, 1024, 1536], P('rep')
- output 3: bfloat16 [2, 1024, 1536], P('rep')
- output 4: bfloat16 [2, 1536, 1024], P('rep')
- output 5: bfloat16 [2, 1024, 4096], P('rep')
- output 6: bfloat16 [2, 1024, 4096], P('rep')
- output 7: bfloat16 [2, 4096, 1024], P('rep')
- output 8: float32 [2, 1024, 1536], P('rep')
- output 9: float32 [2, 1024, 1536], P('rep')
- output 10: float32 [2, 1024, 1536], P('rep')
- output 11: float32 [2, 1536, 1024], P('rep')
- output 12: float32 [2, 1024, 4096], P('rep')
- output 13: float32 [2, 1024, 4096], P('rep')
- output 14: float32 [2, 4096, 1024], P('rep')
- output 15: float32 [2, 1024, 1536], P('rep')
- output 16: float32 [2, 1024, 1536], P('rep')
- output 17: float32 [2, 1024, 1536], P('rep')
- output 18: float32 [2, 1536, 1024], P('rep')
- output 19: float32 [2, 1024, 4096], P('rep')
- output 20: float32 [2, 1024, 4096], P('rep')
- output 21: float32 [2, 4096, 1024], P('rep')
All inputs are finite; a program needn't handle non-finite values.
Results may differ from the reference program's by a relative error of at most 0.0262.
Values are sent between devices in bfloat16 or wider.
A program may use at most 3.25 GiB of HBM per device.

```python
import jax
import jax.numpy as jnp
from jax import lax

SEQUENCES = 8
TOKENS = 2048
D = 1024
HEADS = 12
KV_HEADS = 12
HEAD = 128
FF = 4096
LAYERS = 2
THETA = 10000
NAMES = ("wq", "wk", "wv", "wo", "w_gate", "w_up", "w_down")
SHAPES = {
    "wq": (LAYERS, D, HEADS * HEAD),
    "wk": (LAYERS, D, KV_HEADS * HEAD),
    "wv": (LAYERS, D, KV_HEADS * HEAD),
    "wo": (LAYERS, HEADS * HEAD, D),
    "w_gate": (LAYERS, D, FF),
    "w_up": (LAYERS, D, FF),
    "w_down": (LAYERS, FF, D),
}


def bump(key, n, height):
    away = (jnp.arange(n, dtype=jnp.int32) - jax.random.randint(key, (), 0, n, jnp.int32)) % n
    return jnp.where(away < n // 8, height, 1.0)


def together(key, own, strength):
    shared = jax.random.normal(key, own.shape[1:], jnp.float32)
    return (own + strength * shared) * lax.rsqrt(1 + strength * strength)


def setup_inputs(seed: int = 0, part: int = 0) -> dict:
    kx, kdy, ka, kb, kz, kf, kh, kl, *keys = jax.random.split(jax.random.key(seed), 8 + 3 * len(NAMES))
    kx, kdy, ka, kb = (jax.random.fold_in(k, part) for k in (kx, kdy, ka, kb))
    kw, km, kv = (keys[i::3] for i in range(3))
    shape = (SEQUENCES, TOKENS, D)
    much_x, much_dy = jax.random.uniform(kz, (2,), jnp.float32, 0.0, 1.0)
    loud = 2.0 ** jax.random.uniform(jax.random.fold_in(kz, 1), (), jnp.float32, -1.0, 2.0)
    layers = 2.0 ** jax.random.uniform(kl, (LAYERS, 1, 1), jnp.float32, -1.0, 1.0)
    times = {"wq": 1.0, "wk": 1.0, "wv": 2.0, "wo": layers, "w_gate": 1.0, "w_up": bump(kh, FF, 4.0), "w_down": layers}
    x = together(ka, jax.random.normal(kx, shape, jnp.float32), much_x) * bump(kf, D, 4.0)
    dy = together(kb, jax.random.normal(kdy, shape, jnp.float32), much_dy)
    drawn = {"x": x.astype(jnp.bfloat16), "dy": (loud * dy * (SEQUENCES * TOKENS) ** -0.5).astype(jnp.bfloat16)}
    for key, name in zip(kw, NAMES, strict=True):
        drawn[name] = (jax.random.normal(key, SHAPES[name], jnp.float32) * SHAPES[name][1] ** -0.5 * times[name]).astype(jnp.bfloat16)
    for key, name in zip(km, NAMES, strict=True):
        drawn[f"m_{name}"] = 0.1 * jax.random.normal(key, SHAPES[name], jnp.float32)
    for key, name in zip(kv, NAMES, strict=True):
        drawn[f"v_{name}"] = jax.random.uniform(key, SHAPES[name], jnp.float32, 0.02, 0.06)
    return drawn


def matmul(a, w):
    return jnp.dot(a, w, preferred_element_type=jnp.float32).astype(jnp.bfloat16)


def normed(h):
    wide = h.astype(jnp.float32)
    scale = lax.rsqrt(jnp.mean(wide**2, -1, keepdims=True) + 1e-6)
    return (wide * scale).astype(jnp.bfloat16)


def turned(t, theta):
    half = t.shape[-1] // 2
    angle = jnp.arange(t.shape[0], dtype=jnp.float32)[:, None] * theta ** (-jnp.arange(half, dtype=jnp.float32) / half)
    cos, sin = jnp.cos(angle)[:, None], jnp.sin(angle)[:, None]
    a, b = t[..., :half].astype(jnp.float32), t[..., half:].astype(jnp.float32)
    return jnp.concatenate([a * cos - b * sin, b * cos + a * sin], -1).astype(jnp.bfloat16)


def seen_by(q, k, v):
    tokens, kv = q.shape[0], k.shape[1]
    q = q.reshape(tokens, kv, -1, q.shape[-1])
    scores = jnp.einsum("tgsd,ugd->gstu", q.astype(jnp.float32), k.astype(jnp.float32)) * q.shape[-1] ** -0.5
    place = jnp.arange(tokens)
    weights = jax.nn.softmax(jnp.where(place[:, None] >= place, scores, -jnp.inf), -1).astype(jnp.bfloat16)
    return jnp.einsum("gstu,ugd->tgsd", weights.astype(jnp.float32), v.astype(jnp.float32)).astype(jnp.bfloat16).reshape(tokens, -1)


def layer(h, w):
    a = normed(h)
    q, k = (turned(matmul(a, w[name]).reshape(h.shape[0], -1, HEAD), THETA) for name in ("wq", "wk"))
    h = h + matmul(seen_by(q, k, matmul(a, w["wv"]).reshape(h.shape[0], -1, HEAD)), w["wo"])
    b = normed(h)
    gate = jnp.dot(b, w["w_gate"], preferred_element_type=jnp.float32)
    up = jnp.dot(b, w["w_up"], preferred_element_type=jnp.float32)
    return h + matmul((jax.nn.silu(gate) * up).astype(jnp.bfloat16), w["w_down"])


def adamw(w, m, v, g):
    m = 0.9 * m + 0.1 * g
    v = 0.95 * v + 0.05 * g * g
    step = m * lax.rsqrt(v + 1e-8) + 0.1 * w
    return (w - 0.02 * step).astype(jnp.bfloat16), m, v


def clipped(gradients, sum_of_squares, count):
    factor = jnp.minimum(1.0, 0.5 * lax.rsqrt(sum_of_squares / count + 1e-30))
    return [g * factor for g in gradients]


def stack(weights, h):
    return lax.scan(lambda h, w: (layer(h, w), None), h, weights)[0]


def reference(x, dy, wq, wk, wv, wo, w_gate, w_up, w_down, m_wq, m_wk, m_wv, m_wo, m_w_gate, m_w_up, m_w_down, v_wq, v_wk, v_wv, v_wo, v_w_gate, v_w_up, v_w_down):
    weights = dict(zip(NAMES, (wq, wk, wv, wo, w_gate, w_up, w_down), strict=True))

    def take(so_far, sequence):
        h, by_y = sequence
        _, back = jax.vjp(stack, weights, h)
        by_weights, by_h = back(by_y)
        return jax.tree.map(lambda total, term: total + term.astype(jnp.float32), so_far, by_weights), by_h

    none_yet = {name: jnp.zeros(w.shape, jnp.float32) for name, w in weights.items()}
    by_weights, by_x = lax.scan(take, none_yet, (x, dy))
    gradients = [by_weights[name].astype(jnp.bfloat16).astype(jnp.float32) for name in NAMES]
    gradients = clipped(gradients, sum(jnp.sum(g * g) for g in gradients), sum(g.size for g in gradients))
    first = (m_wq, m_wk, m_wv, m_wo, m_w_gate, m_w_up, m_w_down)
    second = (v_wq, v_wk, v_wv, v_wo, v_w_gate, v_w_up, v_w_down)
    new = [adamw(weights[name].astype(jnp.float32), m, v, g) for name, m, v, g in zip(NAMES, first, second, gradients, strict=True)]
    return tuple(one[which] for which in range(3) for one in new)
```

```python
import functools

import jax
import jax.numpy as jnp
from jax import lax
from jax.experimental import pallas as pl
from jax.experimental.pallas import tpu as pltpu
from jax.sharding import PartitionSpec as P

NEG = -1e30
HIDDEN = 2 * NEG
LOG2E = 1.4426950408889634
VMEM = 58 * 2**20
HEAD = 128
THETA = 10000
NAMES = ("wq", "wk", "wv", "wo", "w_gate", "w_up", "w_down")
BF = jnp.bfloat16
F32 = jnp.float32


def _dot(a, b, ca, cb):
    return lax.dot_general(a, b, (((ca,), (cb,)), ((), ())), preferred_element_type=F32)


def _turn(x, cos, sin):
    return x * cos + pltpu.roll(x, HEAD // 2, 1) * sin


def _gap(bk, bq):
    return lax.broadcasted_iota(jnp.int32, (bk, bq), 1) - lax.broadcasted_iota(jnp.int32, (bk, bq), 0)


def _lanes(i):
    return slice(i * HEAD, (i + 1) * HEAD)


def _spans(iq, bq, bk):
    return lax.div(iq * bq + 1, bk), lax.div(iq * bq + bq - 1 + bk, bk)


def _forward(q_ref, k_ref, v_ref, cos_ref, sin_ref, o_ref, lse_ref, q_s, k_s, v_s, top_s, mix_s, gap_s, *, kb, bq, bk, scale):
    iq = pl.program_id(1)
    tokens = k_ref.shape[0]
    e = scale * LOG2E

    @pl.when(iq == 0)
    def _():
        gap_s[...] = _gap(bk, bq)

        def fill(j, _):
            here = pl.ds(pl.multiple_of(j * 256, 256), 256)
            cos, sin = cos_ref[here, :], sin_ref[here, :]
            for i in range(kb):
                k_s[here, _lanes(i)] = _turn(k_ref[here, _lanes(i)].astype(F32), cos, sin).astype(BF)
                v_s[i, :HEAD, here] = v_ref[here, _lanes(i)].T
                v_s[i, HEAD:, here] = jnp.ones((8, 256), BF)

        lax.fori_loop(0, tokens // 256, fill, None)

    mine = pl.ds(pl.multiple_of(iq * bq, bq), bq)
    cos, sin = cos_ref[mine, :], sin_ref[mine, :]
    for i in range(kb):
        q_s[:, _lanes(i)] = _turn(q_ref[:, _lanes(i)].astype(F32), cos, sin).astype(BF)
    top_s[...] = jnp.full(top_s.shape, NEG, F32)
    mix_s[...] = jnp.zeros(mix_s.shape, F32)

    def block(j, masked):
        here = pl.ds(pl.multiple_of(j * bk, bk), bk)
        scores = [_dot(k_s[here, _lanes(i)], q_s[:, _lanes(i)], 1, 1) for i in range(kb)]
        ok = gap_s[...] >= j * bk - iq * bq if masked else None
        weights, keeps = [], []
        for i, s in enumerate(scores):
            if masked:
                s = jnp.where(ok, s, HIDDEN)
            old = top_s[i : i + 1, :]
            top = jnp.maximum(old, s.max(axis=0, keepdims=True))
            top_s[i : i + 1, :] = top
            weights.append(jnp.exp2((s - top) * e).astype(BF))
            keeps.append(jnp.exp2((old - top) * e))
        for i, (p, keep) in enumerate(zip(weights, keeps)):
            mix_s[i] = mix_s[i] * keep + _dot(v_s[i, :, here], p, 1, 0)

    whole, last = _spans(iq, bq, bk)
    lax.fori_loop(0, whole, lambda j, _: block(j, False), None)
    lax.fori_loop(whole, last, lambda j, _: block(j, True), None)
    for i in range(kb):
        top, total = top_s[i : i + 1, :], mix_s[i, HEAD : HEAD + 1, :]
        o_ref[:, _lanes(i)] = (mix_s[i, :HEAD, :] * (1 / total)).T.astype(BF)
        lse_ref[i] = top * scale + jnp.log(total)


def attend(q, k, v, cos, sin, kb=12, bq=256, bk=512):
    tokens, width = q.shape
    heads = width // HEAD
    rows = lambda n: pl.BlockSpec((n, kb * HEAD), lambda ih, iq: (iq if n == bq else 0, ih))
    table = pl.BlockSpec((tokens, HEAD), lambda ih, iq: (0, 0))
    return pl.pallas_call(
        functools.partial(_forward, kb=kb, bq=bq, bk=bk, scale=HEAD**-0.5),
        grid=(heads // kb, tokens // bq),
        in_specs=[rows(bq), rows(tokens), rows(tokens), table, table],
        out_specs=[rows(bq), pl.BlockSpec((kb, 1, bq), lambda ih, iq: (ih, 0, iq))],
        scratch_shapes=[pltpu.VMEM((bq, kb * HEAD), BF), pltpu.VMEM((tokens, kb * HEAD), BF), pltpu.VMEM((kb, HEAD + 8, tokens), BF),
                        pltpu.VMEM((kb, bq), F32), pltpu.VMEM((kb, HEAD + 8, bq), F32), pltpu.VMEM((bk, bq), jnp.int32)],
        out_shape=[jax.ShapeDtypeStruct((tokens, width), BF), jax.ShapeDtypeStruct((heads, 1, tokens), F32)],
        compiler_params=pltpu.CompilerParams(dimension_semantics=("arbitrary", "arbitrary"), vmem_limit_bytes=VMEM),
        cost_estimate=pl.CostEstimate(flops=4 * tokens * tokens * width, transcendentals=heads * tokens * tokens, bytes_accessed=8 * tokens * width),
        name="attend",
    )(q, k, v, cos, sin)


def _backward(q_ref, k_ref, v_ref, do_ref, o_ref, lse_ref, cos_ref, sin_ref, d_ref,
              q_s, k_s, dq_s, dk_s, dv_s, gap_s, *, kb, bq, bk, scale):
    iq = pl.program_id(1)
    tokens = k_ref.shape[0]
    e = scale * LOG2E

    @pl.when(iq == 0)
    def _():
        gap_s[...] = _gap(bk, bq)
        dk_s[...] = jnp.zeros_like(dk_s)
        dv_s[...] = jnp.zeros_like(dv_s)

        def fill(j, _):
            here = pl.ds(pl.multiple_of(j * 256, 256), 256)
            cos, sin = cos_ref[here, :], sin_ref[here, :]
            for i in range(kb):
                k_s[here, _lanes(i)] = _turn(k_ref[here, _lanes(i)].astype(F32), cos, sin).astype(BF)

        lax.fori_loop(0, tokens // 256, fill, None)

    mine = pl.ds(pl.multiple_of(iq * bq, bq), bq)
    cos, sin = cos_ref[mine, :], sin_ref[mine, :]
    for i in range(kb):
        q_s[:, _lanes(i)] = _turn(q_ref[:, _lanes(i)].astype(F32), cos, sin).astype(BF)
    dq_s[...] = jnp.zeros_like(dq_s)
    lses = [lse_ref[i] * LOG2E for i in range(kb)]
    deltas = [(do_ref[:, _lanes(i)].astype(F32) * o_ref[:, _lanes(i)].astype(F32)).T.sum(axis=0, keepdims=True) for i in range(kb)]

    def block(j, masked):
        here = pl.ds(pl.multiple_of(j * bk, bk), bk)
        qs = [q_s[:, _lanes(i)] for i in range(kb)]
        dos = [do_ref[:, _lanes(i)] for i in range(kb)]
        scores = [_dot(k_s[here, _lanes(i)], qs[i], 1, 1) for i in range(kb)]
        dps = [_dot(v_ref[here, _lanes(i)], dos[i], 1, 1) for i in range(kb)]
        ok = gap_s[...] >= j * bk - iq * bq if masked else None
        for i in range(kb):
            p = jnp.exp2(scores[i] * e - lses[i])
            if masked:
                p = jnp.where(ok, p, 0.0)
            ds = (p * (dps[i] - deltas[i])).astype(BF)
            dv_s[here, _lanes(i)] += _dot(p.astype(BF), dos[i], 1, 0)
            dk_s[here, _lanes(i)] += _dot(ds, qs[i], 1, 0)
            dq_s[i] += _dot(k_s[here, _lanes(i)].T, ds, 1, 0)

    whole, last = _spans(iq, bq, bk)
    lax.fori_loop(0, whole, lambda j, _: block(j, False), None)
    lax.fori_loop(whole, last, lambda j, _: block(j, True), None)
    for i in range(kb):
        dq = (dq_s[i] * scale).T.astype(BF).astype(F32)
        d_ref[0, mine, _lanes(i)] = _turn(dq, cos, -sin).astype(BF)

    @pl.when(iq == pl.num_programs(1) - 1)
    def _():
        def leave(j, _):
            here = pl.ds(pl.multiple_of(j * 256, 256), 256)
            cos, sin = cos_ref[here, :], sin_ref[here, :]
            for i in range(kb):
                dk = (dk_s[here, _lanes(i)] * scale).astype(BF).astype(F32)
                d_ref[1, here, _lanes(i)] = _turn(dk, cos, -sin).astype(BF)
                d_ref[2, here, _lanes(i)] = dv_s[here, _lanes(i)].astype(BF)

        lax.fori_loop(0, tokens // 256, leave, None)


def attend_bwd(q, k, v, d_out, out, lse, cos, sin, kb=4, bq=512, bk=512):
    tokens, width = q.shape
    heads = width // HEAD
    rows = lambda n: pl.BlockSpec((n, kb * HEAD), lambda ih, iq: (iq if n == bq else 0, ih))
    table = pl.BlockSpec((tokens, HEAD), lambda ih, iq: (0, 0))
    return pl.pallas_call(
        functools.partial(_backward, kb=kb, bq=bq, bk=bk, scale=HEAD**-0.5),
        grid=(heads // kb, tokens // bq),
        in_specs=[rows(bq), rows(tokens), rows(tokens), rows(bq), rows(bq), pl.BlockSpec((kb, 1, bq), lambda ih, iq: (ih, 0, iq)), table, table],
        out_specs=pl.BlockSpec((3, tokens, kb * HEAD), lambda ih, iq: (0, 0, ih)),
        scratch_shapes=[pltpu.VMEM((bq, kb * HEAD), BF), pltpu.VMEM((tokens, kb * HEAD), BF), pltpu.VMEM((kb, HEAD, bq), F32),
                        pltpu.VMEM((tokens, kb * HEAD), F32), pltpu.VMEM((tokens, kb * HEAD), F32), pltpu.VMEM((bk, bq), jnp.int32)],
        out_shape=jax.ShapeDtypeStruct((3, tokens, width), BF),
        compiler_params=pltpu.CompilerParams(dimension_semantics=("arbitrary", "arbitrary"), vmem_limit_bytes=VMEM),
        cost_estimate=pl.CostEstimate(flops=10 * tokens * tokens * width, transcendentals=heads * tokens * tokens, bytes_accessed=16 * tokens * width),
        name="attend_bwd",
    )(q, k, v, d_out, out, lse, cos, sin)


def _mlp(b_ref, wg_ref, wu_ref, gate_ref, up_ref, act_ref, *, tm):
    here = pl.ds(pl.multiple_of(pl.program_id(1) * tm, tm), tm)
    b = b_ref[here, :]
    gate, up = _dot(b, wg_ref[...], 1, 0), _dot(b, wu_ref[...], 1, 0)
    gate_ref[...], up_ref[...] = gate, up
    act_ref[...] = (gate * jax.nn.sigmoid(gate) * up).astype(BF)


def mlp(b, w_gate, w_up, n, tm=512, tn=512):
    (tokens, d), ff = b.shape, w_gate.shape[2]
    tile = pl.BlockSpec((tm, tn), lambda j, i: (i, j))
    weight = pl.BlockSpec((None, d, tn), lambda j, i: (n, 0, j))
    return pl.pallas_call(
        functools.partial(_mlp, tm=tm),
        grid=(ff // tn, tokens // tm),
        in_specs=[pl.BlockSpec((tokens, d), lambda j, i: (0, 0)), weight, weight],
        out_specs=[tile] * 3,
        out_shape=[jax.ShapeDtypeStruct((tokens, ff), t) for t in (F32, F32, BF)],
        compiler_params=pltpu.CompilerParams(dimension_semantics=("arbitrary", "arbitrary"), vmem_limit_bytes=VMEM),
        cost_estimate=pl.CostEstimate(flops=4 * tokens * d * ff, transcendentals=tokens * ff, bytes_accessed=10 * tokens * ff + 4 * d * ff),
        name="mlp",
    )(b, w_gate, w_up)


def _mlp_bwd(d_ref, w_ref, gate_ref, up_ref, out_ref, *, tm):
    here = pl.ds(pl.multiple_of(pl.program_id(1) * tm, tm), tm)
    d_act = _dot(d_ref[here, :], w_ref[...], 1, 1).astype(BF).astype(F32)
    gate = gate_ref[...]
    s = jax.nn.sigmoid(gate)
    out_ref[0] = (d_act * up_ref[...] * (s * (1 + gate * (1 - s)))).astype(BF)
    out_ref[1] = (d_act * (gate * s)).astype(BF)


def mlp_inner_bwd(d, w_down, gate, up, n, tm=512, tn=512):
    (tokens, width), ff = d.shape, w_down.shape[1]
    tile = pl.BlockSpec((tm, tn), lambda j, i: (i, j))
    return pl.pallas_call(
        functools.partial(_mlp_bwd, tm=tm),
        grid=(ff // tn, tokens // tm),
        in_specs=[pl.BlockSpec((tokens, width), lambda j, i: (0, 0)), pl.BlockSpec((None, tn, width), lambda j, i: (n, j, 0)), tile, tile],
        out_specs=pl.BlockSpec((2, tm, tn), lambda j, i: (0, i, j)),
        out_shape=jax.ShapeDtypeStruct((2, tokens, ff), BF),
        compiler_params=pltpu.CompilerParams(dimension_semantics=("arbitrary", "arbitrary"), vmem_limit_bytes=VMEM),
        cost_estimate=pl.CostEstimate(flops=2 * tokens * width * ff, transcendentals=tokens * ff, bytes_accessed=12 * tokens * ff),
        name="mlp_bwd",
    )(d, w_down, gate, up)


def _grads(a_ref, d_ref, c_ref, e_ref, out_ref, left_s, *, first):
    s = pl.program_id(0)

    @pl.when(s == 0)
    def _():
        left_s[...] = a_ref[...].T

    @pl.when(s == first)
    def _():
        left_s[...] = c_ref[...].T

    @pl.when(s < first)
    def _():
        out_ref[...] = _dot(left_s[...], d_ref[...], 1, 0).astype(BF)

    @pl.when(s >= first)
    def _():
        out_ref[...] = _dot(left_s[...], e_ref[...], 1, 0).astype(BF)


def grads(a, d, c, e, tn=512):
    (tokens, rows), (parts, _, n) = a.shape, d.shape
    f = n // tn
    first = parts * f
    whole = pl.BlockSpec((tokens, rows), lambda s: (0, 0))
    return pl.pallas_call(
        functools.partial(_grads, first=first),
        grid=(first + f,),
        in_specs=[whole, pl.BlockSpec((None, tokens, tn), lambda s: (jnp.minimum(s, first - 1) // f, 0, jnp.minimum(s, first - 1) % f)),
                  whole, pl.BlockSpec((tokens, tn), lambda s: (0, jnp.maximum(s - first, 0)))],
        out_specs=pl.BlockSpec((rows, tn), lambda s: (0, s)),
        out_shape=jax.ShapeDtypeStruct((rows, (parts + 1) * n), BF),
        scratch_shapes=[pltpu.VMEM((rows, tokens), BF)],
        compiler_params=pltpu.CompilerParams(dimension_semantics=("arbitrary",), vmem_limit_bytes=VMEM),
        cost_estimate=pl.CostEstimate(flops=2 * tokens * rows * (parts + 1) * n, transcendentals=0, bytes_accessed=2 * (tokens + rows) * (parts + 1) * n),
        name="grads",
    )(a, d, c, e)


def _update(factor_ref, *refs, count):
    factor = factor_ref[0]
    old, new = refs[count : 4 * count], refs[-3 * count :]
    for i in range(count):
        g = refs[i][...].astype(F32)
        g = (g.T if i == count - 1 else g) * factor
        w, m, v = (old[3 * i + j][...] for j in range(3))
        m = 0.9 * m + 0.1 * g
        v = 0.95 * v + 0.05 * g * g
        w = w.astype(F32)
        new[3 * i][...] = (w - 0.02 * (m * lax.rsqrt(v + 1e-8) + 0.1 * w)).astype(BF)
        new[3 * i + 1][...] = m
        new[3 * i + 2][...] = v


def update(factor, g, state, n, before, cut):
    count, (down, across) = len(state) // 3, cut
    steps = down * across
    specs, blocks, at = [], [], 0
    for i, x in enumerate(state):
        _, r, c = x.shape
        if i < 3 * (count - 1):
            blocks.append(pl.BlockSpec((None, r // steps, c), lambda s: (n, s, 0)))
            if i % 3 == 0:
                specs.append(pl.BlockSpec((r // steps, c), lambda s, at=at // c: (s, at)))
                at += c
        else:
            blocks.append(pl.BlockSpec((None, r // down, c // across), lambda s: (n, s // across, s % across)))
            if i % 3 == 0:
                specs.append(pl.BlockSpec((c // across, r // down), lambda s, at=at // (r // down): (s % across, at + s // across)))
    held = [] if before is None else list(before)
    return pl.pallas_call(
        functools.partial(_update, count=count),
        grid=(steps,),
        in_specs=[pl.BlockSpec(memory_space=pltpu.SMEM), *specs, *blocks, *[pl.BlockSpec(memory_space=pl.ANY)] * len(held)],
        out_specs=blocks,
        out_shape=[jax.ShapeDtypeStruct(x.shape, x.dtype) for x in state],
        input_output_aliases={1 + count + 3 * count + j: j for j in range(len(held))},
        compiler_params=pltpu.CompilerParams(dimension_semantics=("arbitrary",), vmem_limit_bytes=VMEM),
        cost_estimate=pl.CostEstimate(flops=15 * g.size, transcendentals=g.size, bytes_accessed=22 * g.size),
        name="update",
    )(factor.reshape(1), *[g] * count, *state, *held)


def matmul(a, w):
    return jnp.dot(a, w, preferred_element_type=F32).astype(BF)


def by_left(d, w):
    return _dot(d, w, 1, 1).astype(BF)


def normed(h):
    wide = h.astype(F32)
    scale = lax.rsqrt(jnp.mean(wide**2, -1, keepdims=True) + 1e-6)
    return (wide * scale).astype(BF)


def normed_bwd(h, d):
    wide, d = h.astype(F32), d.astype(F32)
    scale = lax.rsqrt(jnp.mean(wide**2, -1, keepdims=True) + 1e-6)
    unit = wide * scale
    return (scale * (d - unit * jnp.mean(d * unit, -1, keepdims=True))).astype(BF)


def tables(tokens):
    half = HEAD // 2
    angle = jnp.arange(tokens, dtype=F32)[:, None] * THETA ** (-jnp.arange(half, dtype=F32) / half)
    cos, sin = jnp.cos(angle), jnp.sin(angle)
    return jnp.concatenate([cos, cos], -1), jnp.concatenate([-sin, sin], -1)


def layer(h, w, whole, n, cos, sin):
    a = normed(h)
    q, k, v = (matmul(a, w[name]) for name in ("wq", "wk", "wv"))
    out, lse = attend(q, k, v, cos, sin)
    mid = h + matmul(out, w["wo"])
    b = normed(mid)
    gate, up, act = mlp(b, whole["w_gate"], whole["w_up"], n)
    return mid + matmul(act, w["w_down"]), (h, a, q, k, v, out, lse, mid, b, gate, up, act)


def mlp_bwd(d, w, whole, n, kept):
    h, a, q, k, v, out, lse, mid, b, gate, up, act = kept
    d_gu = mlp_inner_bwd(d, whole["w_down"], gate, up, n)
    d_b = by_left(d_gu[0], w["w_gate"]) + by_left(d_gu[1], w["w_up"])
    return d + normed_bwd(mid, d_b), grads(b, d_gu, d, act)


def attention_bwd(d_mid, w, kept, cos, sin):
    h, a, q, k, v, out, lse, mid, b, gate, up, act = kept
    return attend_bwd(q, k, v, by_left(d_mid, w["wo"]), out, lse, cos, sin)


def input_bwd(d_mid, d, w, h):
    d_a = by_left(d[0], w["wq"]) + by_left(d[1], w["wk"]) + by_left(d[2], w["wv"])
    return d_mid + normed_bwd(h, d_a)


MLP, ATTENTION = ("w_gate", "w_up", "w_down"), ("wq", "wk", "wv", "wo")


def solution(mesh):
    tie = lax.optimization_barrier

    def scatter(g):
        return lax.psum_scatter(g, "dp", scatter_dimension=0, tiled=True)

    def gather(g):
        return lax.all_gather(g, "dp", axis=0, tiled=True)

    def step(x, dy, *arrays):
        weights, m, v = (dict(zip(NAMES, arrays[i : i + 7], strict=True)) for i in (0, 7, 14))
        count = weights["wq"].shape[0]
        layers = [{name: w[n] for name, w in weights.items()} for n in range(count)]
        cos, sin = tables(x.shape[1])
        h, kept = x[0], []
        for n, w in enumerate(layers):
            h, some = layer(h, w, weights, n, cos, sin)
            kept.append(some)
        d = dy[0]
        shards, full = {}, {}
        for n in reversed(range(count)):
            w, some = layers[n], kept[n]
            d_mid, g = mlp_bwd(d, w, weights, n, some)
            d_mid, g = tie((d_mid, g))
            shards[n, MLP] = scatter(g)
            if n < count - 1:
                d_mid, full[n + 1, MLP] = tie((d_mid, full[n + 1, MLP]))
            d = attention_bwd(d_mid, w, some, cos, sin)
            if n > 0:
                d, shards[n, MLP] = tie((d, shards[n, MLP]))
                full[n, MLP] = gather(shards[n, MLP])
            g = grads(some[1], d, d_mid, some[5])
            if n > 0:
                d = input_bwd(d_mid, d, w, some[0])
                d, g = tie((d, g))
            shards[n, ATTENTION] = scatter(g)
        total = lax.psum(sum(jnp.sum(jnp.square(s.astype(F32))) for s in shards.values()), "dp")
        size = sum(w.size for w in weights.values())
        factor = jnp.minimum(1.0, 0.5 * lax.rsqrt(total / size + 1e-30))
        got = {MLP: None, ATTENTION: None}
        for part, cut in ((MLP, (32, 1)), (ATTENTION, (4, 4))):
            state = [of[name] for name in part for of in (weights, m, v)]
            for n in reversed(range(count)):
                if (n, part) not in full:
                    full[n, part] = gather(shards[n, part])
                got[part] = update(factor, full[n, part], state, n, got[part], cut)
                factor, got[part] = tie((factor, got[part]))
        new = {name: got[part][3 * i : 3 * i + 3] for part in got for i, name in enumerate(part)}
        return tuple(new[name][which] for which in range(3) for name in NAMES)

    states, all_of = P(("rep", "dp"), None, None), P(None, None, None)
    return jax.shard_map(
        step,
        mesh=mesh,
        in_specs=(states, states) + (all_of,) * 21,
        out_specs=(P("rep", None, None),) * 21,
        check_vma=False,
    )
```

```python
import functools

import jax
import jax.numpy as jnp
from jax import lax
from jax.experimental import pallas as pl
from jax.experimental.pallas import tpu as pltpu
from jax.sharding import PartitionSpec as P

NEG = -1e30
HIDDEN = 2 * NEG
LOG2E = 1.4426950408889634
VMEM = 58 * 2**20
HEAD = 128
THETA = 10000
NAMES = ("wq", "wk", "wv", "wo", "w_gate", "w_up", "w_down")
BF = jnp.bfloat16
F32 = jnp.float32


def _dot(a, b, ca, cb):
    return lax.dot_general(a, b, (((ca,), (cb,)), ((), ())), preferred_element_type=F32)


def _turn(x, cos, sin):
    return x * cos + pltpu.roll(x, HEAD // 2, 1) * sin


def _gap(bk, bq):
    return lax.broadcasted_iota(jnp.int32, (bk, bq), 1) - lax.broadcasted_iota(jnp.int32, (bk, bq), 0)


def _lanes(i):
    return slice(i * HEAD, (i + 1) * HEAD)


def _forward(q_ref, k_ref, v_ref, cos_ref, sin_ref, o_ref, lse_ref, q_s, k_s, v_s, top_s, mix_s, gap_s, *, kb, bq, bk, scale):
    iq = pl.program_id(1)
    tokens = k_ref.shape[0]
    e = scale * LOG2E

    @pl.when(iq == 0)
    def _():
        gap_s[...] = _gap(bq, bq)

        def fill(j, _):
            here = pl.ds(pl.multiple_of(j * 256, 256), 256)
            cos, sin = cos_ref[here, :], sin_ref[here, :]
            for i in range(kb):
                k_s[here, _lanes(i)] = _turn(k_ref[here, _lanes(i)].astype(F32), cos, sin).astype(BF)
                v_s[i, :HEAD, here] = v_ref[here, _lanes(i)].T
                v_s[i, HEAD:, here] = jnp.ones((8, 256), BF)

        lax.fori_loop(0, tokens // 256, fill, None)

    mine = pl.ds(pl.multiple_of(iq * bq, bq), bq)
    cos, sin = cos_ref[mine, :], sin_ref[mine, :]
    for i in range(kb):
        q_s[:, _lanes(i)] = _turn(q_ref[:, _lanes(i)].astype(F32), cos, sin).astype(BF)
    top_s[...] = jnp.full(top_s.shape, NEG, F32)
    mix_s[...] = jnp.zeros(mix_s.shape, F32)

    def block(start, size, masked):
        here = pl.ds(pl.multiple_of(start, size), size)
        scores = [_dot(k_s[here, _lanes(i)], q_s[:, _lanes(i)], 1, 1) for i in range(kb)]
        ok = gap_s[...] >= 0 if masked else None
        weights, keeps = [], []
        for i, s in enumerate(scores):
            if masked:
                s = jnp.where(ok, s, HIDDEN)
            old = top_s[i : i + 1, :]
            top = jnp.maximum(old, s.max(axis=0, keepdims=True))
            top_s[i : i + 1, :] = top
            weights.append(jnp.exp2((s - top) * e).astype(BF))
            keeps.append(jnp.exp2((old - top) * e))
        for i, (p, keep) in enumerate(zip(weights, keeps)):
            mix_s[i] = mix_s[i] * keep + _dot(v_s[i, :, here], p, 1, 0)

    whole = lax.div(iq * bq, bk)
    lax.fori_loop(0, whole, lambda j, _: block(j * bk, bk, False), None)
    lax.fori_loop(whole * (bk // bq), iq, lambda j, _: block(j * bq, bq, False), None)
    block(iq * bq, bq, True)
    for i in range(kb):
        top, total = top_s[i : i + 1, :], mix_s[i, HEAD : HEAD + 1, :]
        o_ref[:, _lanes(i)] = (mix_s[i, :HEAD, :] * (1 / total)).T.astype(BF)
        lse_ref[i] = top * scale + jnp.log(total)


def attend(q, k, v, cos, sin, kb=12, bq=256, bk=512):
    tokens, width = q.shape
    heads = width // HEAD
    rows = lambda n: pl.BlockSpec((n, kb * HEAD), lambda ih, iq: (iq if n == bq else 0, ih))
    table = pl.BlockSpec((tokens, HEAD), lambda ih, iq: (0, 0))
    return pl.pallas_call(
        functools.partial(_forward, kb=kb, bq=bq, bk=bk, scale=HEAD**-0.5),
        grid=(heads // kb, tokens // bq),
        in_specs=[rows(bq), rows(tokens), rows(tokens), table, table],
        out_specs=[rows(bq), pl.BlockSpec((kb, 1, bq), lambda ih, iq: (ih, 0, iq))],
        scratch_shapes=[pltpu.VMEM((bq, kb * HEAD), BF), pltpu.VMEM((tokens, kb * HEAD), BF), pltpu.VMEM((kb, HEAD + 8, tokens), BF),
                        pltpu.VMEM((kb, bq), F32), pltpu.VMEM((kb, HEAD + 8, bq), F32), pltpu.VMEM((bq, bq), jnp.int32)],
        out_shape=[jax.ShapeDtypeStruct((tokens, width), BF), jax.ShapeDtypeStruct((heads, 1, tokens), F32)],
        compiler_params=pltpu.CompilerParams(dimension_semantics=("arbitrary", "arbitrary"), vmem_limit_bytes=VMEM),
        cost_estimate=pl.CostEstimate(flops=4 * tokens * tokens * width, transcendentals=heads * tokens * tokens, bytes_accessed=8 * tokens * width),
        name="attend",
    )(q, k, v, cos, sin)


def _backward(q_ref, k_ref, v_ref, do_ref, o_ref, lse_ref, cos_ref, sin_ref, d_ref,
              q_s, k_s, dq_s, dk_s, dv_s, gap_s, *, kb, bq, bk, scale):
    iq = pl.program_id(1)
    tokens = k_ref.shape[0]
    e = scale * LOG2E

    @pl.when(iq == 0)
    def _():
        gap_s[...] = _gap(bk, bq)
        dk_s[...] = jnp.zeros_like(dk_s)
        dv_s[...] = jnp.zeros_like(dv_s)

        def fill(j, _):
            here = pl.ds(pl.multiple_of(j * 256, 256), 256)
            cos, sin = cos_ref[here, :], sin_ref[here, :]
            for i in range(kb):
                k_s[here, _lanes(i)] = _turn(k_ref[here, _lanes(i)].astype(F32), cos, sin).astype(BF)

        lax.fori_loop(0, tokens // 256, fill, None)

    mine = pl.ds(pl.multiple_of(iq * bq, bq), bq)
    cos, sin = cos_ref[mine, :], sin_ref[mine, :]
    for i in range(kb):
        q_s[:, _lanes(i)] = _turn(q_ref[:, _lanes(i)].astype(F32), cos, sin).astype(BF)
    dq_s[...] = jnp.zeros_like(dq_s)
    lses = [lse_ref[i] * LOG2E for i in range(kb)]
    deltas = [(do_ref[:, _lanes(i)].astype(F32) * o_ref[:, _lanes(i)].astype(F32)).T.sum(axis=0, keepdims=True) for i in range(kb)]

    def block(start, size, first, masked):
        here = pl.ds(pl.multiple_of(start, size), size)
        qs = [q_s[first:, _lanes(i)] for i in range(kb)]
        dos = [do_ref[first:, _lanes(i)] for i in range(kb)]
        scores = [_dot(k_s[here, _lanes(i)], qs[i], 1, 1) for i in range(kb)]
        dps = [_dot(v_ref[here, _lanes(i)], dos[i], 1, 1) for i in range(kb)]
        ok = gap_s[:, : bq - first] >= 0 if masked else None
        for i in range(kb):
            p = jnp.exp2(scores[i] * e - lses[i][:, first:])
            if masked:
                p = jnp.where(ok, p, 0.0)
            ds = (p * (dps[i] - deltas[i][:, first:])).astype(BF)
            dv_s[here, _lanes(i)] += _dot(p.astype(BF), dos[i], 1, 0)
            dk_s[here, _lanes(i)] += _dot(ds, qs[i], 1, 0)
            dq_s[i, :, first:] += _dot(k_s[here, _lanes(i)].T, ds, 1, 0)

    lax.fori_loop(0, iq, lambda j, _: block(j * bq, bq, 0, False), None)
    for first in range(0, bq, bk):
        block(iq * bq + first, bk, first, True)
    for i in range(kb):
        dq = (dq_s[i] * scale).T.astype(BF).astype(F32)
        d_ref[0, mine, _lanes(i)] = _turn(dq, cos, -sin).astype(BF)

    @pl.when(iq == pl.num_programs(1) - 1)
    def _():
        def leave(j, _):
            here = pl.ds(pl.multiple_of(j * 256, 256), 256)
            cos, sin = cos_ref[here, :], sin_ref[here, :]
            for i in range(kb):
                dk = (dk_s[here, _lanes(i)] * scale).astype(BF).astype(F32)
                d_ref[1, here, _lanes(i)] = _turn(dk, cos, -sin).astype(BF)
                d_ref[2, here, _lanes(i)] = dv_s[here, _lanes(i)].astype(BF)

        lax.fori_loop(0, tokens // 256, leave, None)


def attend_bwd(q, k, v, d_out, out, lse, cos, sin, kb=4, bq=512, bk=256):
    tokens, width = q.shape
    heads = width // HEAD
    rows = lambda n: pl.BlockSpec((n, kb * HEAD), lambda ih, iq: (iq if n == bq else 0, ih))
    table = pl.BlockSpec((tokens, HEAD), lambda ih, iq: (0, 0))
    return pl.pallas_call(
        functools.partial(_backward, kb=kb, bq=bq, bk=bk, scale=HEAD**-0.5),
        grid=(heads // kb, tokens // bq),
        in_specs=[rows(bq), rows(tokens), rows(tokens), rows(bq), rows(bq), pl.BlockSpec((kb, 1, bq), lambda ih, iq: (ih, 0, iq)), table, table],
        out_specs=pl.BlockSpec((3, tokens, kb * HEAD), lambda ih, iq: (0, 0, ih)),
        scratch_shapes=[pltpu.VMEM((bq, kb * HEAD), BF), pltpu.VMEM((tokens, kb * HEAD), BF), pltpu.VMEM((kb, HEAD, bq), F32),
                        pltpu.VMEM((tokens, kb * HEAD), F32), pltpu.VMEM((tokens, kb * HEAD), F32), pltpu.VMEM((bk, bq), jnp.int32)],
        out_shape=jax.ShapeDtypeStruct((3, tokens, width), BF),
        compiler_params=pltpu.CompilerParams(dimension_semantics=("arbitrary", "arbitrary"), vmem_limit_bytes=VMEM),
        cost_estimate=pl.CostEstimate(flops=10 * tokens * tokens * width, transcendentals=heads * tokens * tokens, bytes_accessed=16 * tokens * width),
        name="attend_bwd",
    )(q, k, v, d_out, out, lse, cos, sin)


def _mlp(b_ref, wg_ref, wu_ref, gate_ref, up_ref, act_ref, *, tm, ch):
    b = b_ref[pl.ds(pl.multiple_of(pl.program_id(1) * tm, tm), tm), :]
    for at in range(0, act_ref.shape[1], ch):
        here = slice(at, at + ch)
        gate, up = _dot(b, wg_ref[:, here], 1, 0), _dot(b, wu_ref[:, here], 1, 0)
        gate_ref[:, here], up_ref[:, here] = gate, up
        act_ref[:, here] = (gate * jax.nn.sigmoid(gate) * up).astype(BF)


def mlp(b, w_gate, w_up, n, tm=2048, tn=256, ch=256):
    (tokens, d), ff = b.shape, w_gate.shape[2]
    tile = pl.BlockSpec((tm, tn), lambda j, i: (i, j))
    weight = pl.BlockSpec((None, d, tn), lambda j, i: (n, 0, j))
    return pl.pallas_call(
        functools.partial(_mlp, tm=tm, ch=ch),
        grid=(ff // tn, tokens // tm),
        in_specs=[pl.BlockSpec((tokens, d), lambda j, i: (0, 0)), weight, weight],
        out_specs=[tile] * 3,
        out_shape=[jax.ShapeDtypeStruct((tokens, ff), t) for t in (F32, F32, BF)],
        compiler_params=pltpu.CompilerParams(dimension_semantics=("arbitrary", "arbitrary"), vmem_limit_bytes=VMEM),
        cost_estimate=pl.CostEstimate(flops=4 * tokens * d * ff, transcendentals=tokens * ff, bytes_accessed=10 * tokens * ff + 4 * d * ff),
        name="mlp",
    )(b, w_gate, w_up)


def _mlp_bwd(d_ref, w_ref, gate_ref, up_ref, out_ref, *, tm, ch):
    d = d_ref[pl.ds(pl.multiple_of(pl.program_id(1) * tm, tm), tm), :]
    for at in range(0, gate_ref.shape[1], ch):
        here = slice(at, at + ch)
        d_act = _dot(d, w_ref[here, :], 1, 1).astype(BF).astype(F32)
        gate = gate_ref[:, here]
        s = jax.nn.sigmoid(gate)
        out_ref[0, :, here] = (d_act * up_ref[:, here] * (s * (1 + gate * (1 - s)))).astype(BF)
        out_ref[1, :, here] = (d_act * (gate * s)).astype(BF)


def mlp_inner_bwd(d, w_down, gate, up, n, tm=512, tn=1024, ch=256):
    (tokens, width), ff = d.shape, w_down.shape[1]
    tile = pl.BlockSpec((tm, tn), lambda j, i: (i, j))
    return pl.pallas_call(
        functools.partial(_mlp_bwd, tm=tm, ch=ch),
        grid=(ff // tn, tokens // tm),
        in_specs=[pl.BlockSpec((tokens, width), lambda j, i: (0, 0)), pl.BlockSpec((None, tn, width), lambda j, i: (n, j, 0)), tile, tile],
        out_specs=pl.BlockSpec((2, tm, tn), lambda j, i: (0, i, j)),
        out_shape=jax.ShapeDtypeStruct((2, tokens, ff), BF),
        compiler_params=pltpu.CompilerParams(dimension_semantics=("arbitrary", "arbitrary"), vmem_limit_bytes=VMEM),
        cost_estimate=pl.CostEstimate(flops=2 * tokens * width * ff, transcendentals=tokens * ff, bytes_accessed=12 * tokens * ff),
        name="mlp_bwd",
    )(d, w_down, gate, up)


def _grads(a_ref, d_ref, c_ref, e_ref, out_ref, left_s, *, first):
    s = pl.program_id(0)

    @pl.when(s == 0)
    def _():
        left_s[...] = a_ref[...].T

    @pl.when(s == first)
    def _():
        left_s[...] = c_ref[...].T

    @pl.when(s < first)
    def _():
        out_ref[...] = _dot(left_s[...], d_ref[...], 1, 0).astype(BF)

    @pl.when(s >= first)
    def _():
        out_ref[...] = _dot(left_s[...], e_ref[...], 1, 0).astype(BF)


def grads(a, d, c, e, tn=512):
    (tokens, rows), (parts, _, n) = a.shape, d.shape
    f = n // tn
    first = parts * f
    whole = pl.BlockSpec((tokens, rows), lambda s: (0, 0))
    return pl.pallas_call(
        functools.partial(_grads, first=first),
        grid=(first + f,),
        in_specs=[whole, pl.BlockSpec((None, tokens, tn), lambda s: (jnp.minimum(s, first - 1) // f, 0, jnp.minimum(s, first - 1) % f)),
                  whole, pl.BlockSpec((tokens, tn), lambda s: (0, jnp.maximum(s - first, 0)))],
        out_specs=pl.BlockSpec((rows, tn), lambda s: (0, s)),
        out_shape=jax.ShapeDtypeStruct((rows, (parts + 1) * n), BF),
        scratch_shapes=[pltpu.VMEM((rows, tokens), BF)],
        compiler_params=pltpu.CompilerParams(dimension_semantics=("arbitrary",), vmem_limit_bytes=VMEM),
        cost_estimate=pl.CostEstimate(flops=2 * tokens * rows * (parts + 1) * n, transcendentals=0, bytes_accessed=2 * (tokens + rows) * (parts + 1) * n),
        name="grads",
    )(a, d, c, e)


def _update(factor_ref, *refs, count):
    factor = factor_ref[0:1, 0:1]
    old, new = refs[count : 4 * count], refs[-3 * count :]
    for i in range(count):
        g = refs[i][...].astype(F32)
        g = (g.T if i == count - 1 else g) * factor
        w, m, v = (old[3 * i + j][...] for j in range(3))
        m = 0.9 * m + 0.1 * g
        v = 0.95 * v + 0.05 * g * g
        w = w.astype(F32)
        new[3 * i][...] = (w - 0.02 * (m * lax.rsqrt(v + 1e-8) + 0.1 * w)).astype(BF)
        new[3 * i + 1][...] = m
        new[3 * i + 2][...] = v


def update(factor, g, state, n, before, cut):
    count, (down, across) = len(state) // 3, cut
    steps = down * across
    specs, blocks, at = [], [], 0
    for i, x in enumerate(state):
        _, r, c = x.shape
        if i < 3 * (count - 1):
            blocks.append(pl.BlockSpec((None, r // steps, c), lambda s: (n, s, 0)))
            if i % 3 == 0:
                specs.append(pl.BlockSpec((r // steps, c), lambda s, at=at // c: (s, at)))
                at += c
        else:
            blocks.append(pl.BlockSpec((None, r // down, c // across), lambda s: (n, s // across, s % across)))
            if i % 3 == 0:
                specs.append(pl.BlockSpec((c // across, r // down), lambda s, at=at // (r // down): (s % across, at + s // across)))
    held = [] if before is None else list(before)
    return pl.pallas_call(
        functools.partial(_update, count=count),
        grid=(steps,),
        in_specs=[pl.BlockSpec((8, 128), lambda s: (0, 0)), *specs, *blocks, *[pl.BlockSpec(memory_space=pl.ANY)] * len(held)],
        out_specs=blocks,
        out_shape=[jax.ShapeDtypeStruct(x.shape, x.dtype) for x in state],
        input_output_aliases={1 + count + 3 * count + j: j for j in range(len(held))},
        compiler_params=pltpu.CompilerParams(dimension_semantics=("arbitrary",), vmem_limit_bytes=VMEM),
        cost_estimate=pl.CostEstimate(flops=15 * g.size, transcendentals=g.size, bytes_accessed=22 * g.size),
        name="update",
    )(factor, *[g] * count, *state, *held)


def _back(d_ref, *refs, parts, per):
    w_refs, (h_ref, by_ref, out_ref, sum_s) = refs[:parts], refs[parts:]
    s = pl.program_id(0)
    for p in range(parts):
        @pl.when(lax.div(s, per) == p)
        def _():
            got = _dot(d_ref[...], w_refs[p][...], 1, 1)
            if p == 0:
                @pl.when(s == 0)
                def _():
                    sum_s[...] = got

                @pl.when(s > 0)
                def _():
                    sum_s[...] += got
            else:
                sum_s[...] += got

    @pl.when(s == pl.num_programs(0) - 1)
    def _():
        def rows(j, _):
            here = pl.ds(pl.multiple_of(j * 256, 256), 256)
            wide, d = h_ref[here, :].astype(F32), sum_s[here, :].astype(BF).astype(F32)
            scale = lax.rsqrt(jnp.mean(wide * wide, -1, keepdims=True) + 1e-6)
            unit = wide * scale
            d = (scale * (d - unit * jnp.mean(d * unit, -1, keepdims=True))).astype(BF)
            out_ref[here, :] = (by_ref[here, :].astype(F32) + d.astype(F32)).astype(BF)

        lax.fori_loop(0, out_ref.shape[0] // 256, rows, None)


def back(d, ws, n, h, by, tk):
    parts, tokens, width = d.shape
    rows = ws[0].shape[1]
    per = width // tk
    whole = pl.BlockSpec((tokens, rows), lambda s: (0, 0))
    weight = lambda p: pl.BlockSpec((None, rows, tk), lambda s: (n, 0, jnp.clip(s - p * per, 0, per - 1)))
    return pl.pallas_call(
        functools.partial(_back, parts=parts, per=per),
        grid=(parts * per,),
        in_specs=[pl.BlockSpec((None, tokens, tk), lambda s: (lax.div(s, per), 0, lax.rem(s, per))), *[weight(p) for p in range(parts)], whole, whole],
        out_specs=whole,
        out_shape=jax.ShapeDtypeStruct((tokens, rows), BF),
        scratch_shapes=[pltpu.VMEM((tokens, rows), F32)],
        compiler_params=pltpu.CompilerParams(dimension_semantics=("arbitrary",), vmem_limit_bytes=VMEM),
        cost_estimate=pl.CostEstimate(flops=2 * tokens * rows * parts * width, transcendentals=tokens, bytes_accessed=2 * (tokens + rows) * parts * width),
        name="back",
    )(d, *ws, h, by)


def _factor(*refs, size):
    shards, (out_ref, mine, got, send, recv) = refs[:-5], refs[-5:]
    n = got.shape[0]
    me = lax.axis_index("dp")
    others = [lax.rem(me + k, n) for k in range(1, n)]
    barrier = pltpu.get_barrier_semaphore()
    for other in others:
        pl.semaphore_signal(barrier, inc=1, device_id={"dp": other}, device_id_type=pl.DeviceIdType.MESH)
    total = jnp.zeros((1, 1), F32)
    for ref in shards:
        for at in range(0, ref.shape[1], 1536):
            def rows(j, so_far):
                x = ref[pl.ds(pl.multiple_of(j * 16, 16), 16), at : at + 1536].astype(F32)
                return so_far + x * x

            part = lax.fori_loop(0, ref.shape[0] // 16, rows, jnp.zeros((16, 1536), F32))
            total += jnp.sum(jnp.sum(part, axis=0, keepdims=True), axis=1, keepdims=True)
    total = jnp.broadcast_to(total, (8, 128))
    mine[...] = total
    got[me] = total
    pl.semaphore_wait(barrier, n - 1)
    copies = [pltpu.make_async_remote_copy(mine, got.at[me], send.at[k], recv.at[k], device_id={"dp": other}, device_id_type=pl.DeviceIdType.MESH)
              for k, other in enumerate(others)]
    for copy in copies:
        copy.start()
    for k, copy in enumerate(copies):
        copy.wait_send()
        source = lax.rem(me + n - 1 - k, n)
        pltpu.make_async_remote_copy(mine, got.at[source], send.at[k], recv.at[k], device_id={"dp": source}, device_id_type=pl.DeviceIdType.MESH).wait_recv()
    total = got[0]
    for i in range(1, n):
        total += got[i]
    out_ref[...] = jnp.minimum(1.0, 0.5 * lax.rsqrt(total / size + 1e-30))


def clip_factor(shards, n, size):
    return pl.pallas_call(
        functools.partial(_factor, size=size),
        in_specs=[pl.BlockSpec(memory_space=pltpu.VMEM)] * len(shards),
        out_specs=pl.BlockSpec(memory_space=pltpu.VMEM),
        out_shape=jax.ShapeDtypeStruct((8, 128), F32),
        scratch_shapes=[pltpu.VMEM((8, 128), F32), pltpu.VMEM((n, 8, 128), F32), pltpu.SemaphoreType.DMA((n - 1,)), pltpu.SemaphoreType.DMA((n - 1,))],
        compiler_params=pltpu.CompilerParams(collective_id=1, has_side_effects=True, vmem_limit_bytes=VMEM),
        cost_estimate=pl.CostEstimate(flops=2 * size // n, transcendentals=0, bytes_accessed=2 * size // n),
        name="clip_factor",
    )(*shards)


def matmul(a, w):
    return jnp.dot(a, w, preferred_element_type=F32).astype(BF)


def by_left(d, w):
    return _dot(d, w, 1, 1).astype(BF)


def normed(h):
    wide = h.astype(F32)
    scale = lax.rsqrt(jnp.mean(wide**2, -1, keepdims=True) + 1e-6)
    return (wide * scale).astype(BF)


def tables(tokens):
    half = HEAD // 2
    angle = jnp.arange(tokens, dtype=F32)[:, None] * THETA ** (-jnp.arange(half, dtype=F32) / half)
    cos, sin = jnp.cos(angle), jnp.sin(angle)
    return jnp.concatenate([cos, cos], -1), jnp.concatenate([-sin, sin], -1)


def layer(h, w, whole, n, cos, sin):
    a = normed(h)
    q, k, v = (matmul(a, w[name]) for name in ("wq", "wk", "wv"))
    out, lse = attend(q, k, v, cos, sin)
    mid = h + matmul(out, w["wo"])
    b = normed(mid)
    gate, up, act = mlp(b, whole["w_gate"], whole["w_up"], n)
    return mid + matmul(act, w["w_down"]), (h, a, q, k, v, out, lse, mid, b, gate, up, act)


MLP, ATTENTION = ("w_gate", "w_up", "w_down"), ("wq", "wk", "wv", "wo")


def solution(mesh):
    tie = lax.optimization_barrier

    def scatter(g):
        return lax.psum_scatter(g, "dp", scatter_dimension=0, tiled=True)

    def gather(g):
        return lax.all_gather(g, "dp", axis=0, tiled=True)

    def step(x, dy, *arrays):
        weights, m, v = (dict(zip(NAMES, arrays[i : i + 7], strict=True)) for i in (0, 7, 14))
        count = weights["wq"].shape[0]
        layers = [{name: w[n] for name, w in weights.items()} for n in range(count)]
        cos, sin = tables(x.shape[1])
        h, kept = x[0], []
        for n, w in enumerate(layers):
            h, some = layer(h, w, weights, n, cos, sin)
            kept.append(some)
        d = dy[0]
        shards, full = {}, {}
        for n in reversed(range(count)):
            h, a, q, k, values, out, lse, mid, b, gate, up, act = kept[n]
            d_gu = mlp_inner_bwd(d, weights["w_down"], gate, up, n)
            d_gu, g = tie((d_gu, grads(b, d_gu, d, act)))
            shards[n, MLP] = scatter(g)
            d_mid = back(d_gu, (weights["w_gate"], weights["w_up"]), n, mid, d, 1024)
            if n < count - 1:
                d_mid, full[n + 1, MLP] = tie((d_mid, full[n + 1, MLP]))
            d = attend_bwd(q, k, values, by_left(d_mid, layers[n]["wo"]), out, lse, cos, sin)
            if n < count - 1:
                d, shards[n + 1, ATTENTION] = tie((d, shards[n + 1, ATTENTION]))
            if n > 0:
                d, shards[n, MLP] = tie((d, shards[n, MLP]))
                full[n, MLP] = gather(shards[n, MLP])
            d, g = tie((d, grads(a, d, d_mid, out)))
            shards[n, ATTENTION] = scatter(g)
            if n > 0:
                d = back(d, tuple(weights[name] for name in ("wq", "wk", "wv")), n, h, d_mid, 768)
        shards = dict(zip(shards, tie(tuple(shards.values()))))
        factor = clip_factor(tuple(shards.values()), mesh.shape["dp"], sum(w.size for w in weights.values()))
        got = {MLP: None, ATTENTION: None}
        for part, cut in ((MLP, (32, 1)), (ATTENTION, (4, 4))):
            state = [of[name] for name in part for of in (weights, m, v)]
            for n in reversed(range(count)):
                if (n, part) not in full:
                    full[n, part] = gather(shards[n, part])
                got[part] = update(factor, full[n, part], state, n, got[part], cut)
                factor, got[part] = tie((factor, got[part]))
        new = {name: got[part][3 * i : 3 * i + 3] for part in got for i, name in enumerate(part)}
        return tuple(new[name][which] for which in range(3) for name in NAMES)

    states, all_of = P(("rep", "dp"), None, None), P(None, None, None)
    return jax.shard_map(
        step,
        mesh=mesh,
        in_specs=(states, states) + (all_of,) * 21,
        out_specs=(P("rep", None, None),) * 21,
        check_vma=False,
    )
```

```python
import functools

import jax
import jax.numpy as jnp
from jax import lax
from jax.experimental import pallas as pl
from jax.experimental.pallas import tpu as pltpu
from jax.sharding import PartitionSpec as P

NEG = -1e30
HIDDEN = 2 * NEG
LOG2E = 1.4426950408889634
VMEM = 58 * 2**20
HEAD = 128
THETA = 10000
NAMES = ("wq", "wk", "wv", "wo", "w_gate", "w_up", "w_down")
BF = jnp.bfloat16
F32 = jnp.float32


def _dot(a, b, ca, cb):
    return lax.dot_general(a, b, (((ca,), (cb,)), ((), ())), preferred_element_type=F32)


def _turn(x, cos, sin):
    return x * cos + pltpu.roll(x, HEAD // 2, 1) * sin


def _gap(bk, bq):
    return lax.broadcasted_iota(jnp.int32, (bk, bq), 1) - lax.broadcasted_iota(jnp.int32, (bk, bq), 0)


def _lanes(i):
    return slice(i * HEAD, (i + 1) * HEAD)


def _forward(q_ref, k_ref, v_ref, cos_ref, sin_ref, o_ref, lse_ref, q_s, k_s, v_s, top_s, mix_s, gap_s, *, kb, bq, bk, scale):
    iq = pl.program_id(1)
    tokens = k_ref.shape[0]
    e = scale * LOG2E

    @pl.when(iq == 0)
    def _():
        gap_s[...] = _gap(bq, bq)

        def fill(j, _):
            here = pl.ds(pl.multiple_of(j * 256, 256), 256)
            cos, sin = cos_ref[here, :], sin_ref[here, :]
            for i in range(kb):
                k_s[here, _lanes(i)] = _turn(k_ref[here, _lanes(i)].astype(F32), cos, sin).astype(BF)
                v_s[i, :HEAD, here] = v_ref[here, _lanes(i)].T
                v_s[i, HEAD:, here] = jnp.ones((8, 256), BF)

        lax.fori_loop(0, tokens // 256, fill, None)

    mine = pl.ds(pl.multiple_of(iq * bq, bq), bq)
    cos, sin = cos_ref[mine, :], sin_ref[mine, :]
    for i in range(kb):
        q_s[:, _lanes(i)] = _turn(q_ref[:, _lanes(i)].astype(F32), cos, sin).astype(BF)
    top_s[...] = jnp.full(top_s.shape, NEG, F32)
    mix_s[...] = jnp.zeros(mix_s.shape, F32)

    def block(start, size, masked):
        here = pl.ds(pl.multiple_of(start, size), size)
        scores = [_dot(k_s[here, _lanes(i)], q_s[:, _lanes(i)], 1, 1) for i in range(kb)]
        ok = gap_s[...] >= 0 if masked else None
        weights, keeps = [], []
        for i, s in enumerate(scores):
            if masked:
                s = jnp.where(ok, s, HIDDEN)
            old = top_s[i : i + 1, :]
            top = jnp.maximum(old, s.max(axis=0, keepdims=True))
            top_s[i : i + 1, :] = top
            weights.append(jnp.exp2((s - top) * e).astype(BF))
            keeps.append(jnp.exp2((old - top) * e))
        for i, (p, keep) in enumerate(zip(weights, keeps)):
            mix_s[i] = mix_s[i] * keep + _dot(v_s[i, :, here], p, 1, 0)

    whole = lax.div(iq * bq, bk)
    lax.fori_loop(0, whole, lambda j, _: block(j * bk, bk, False), None)
    lax.fori_loop(whole * (bk // bq), iq, lambda j, _: block(j * bq, bq, False), None)
    block(iq * bq, bq, True)
    for i in range(kb):
        top, total = top_s[i : i + 1, :], mix_s[i, HEAD : HEAD + 1, :]
        o_ref[:, _lanes(i)] = (mix_s[i, :HEAD, :] * (1 / total)).T.astype(BF)
        lse_ref[i] = top * scale + jnp.log(total)


def attend(q, k, v, cos, sin, kb=12, bq=256, bk=512):
    tokens, width = q.shape
    heads = width // HEAD
    rows = lambda n: pl.BlockSpec((n, kb * HEAD), lambda ih, iq: (iq if n == bq else 0, ih))
    table = pl.BlockSpec((tokens, HEAD), lambda ih, iq: (0, 0))
    return pl.pallas_call(
        functools.partial(_forward, kb=kb, bq=bq, bk=bk, scale=HEAD**-0.5),
        grid=(heads // kb, tokens // bq),
        in_specs=[rows(bq), rows(tokens), rows(tokens), table, table],
        out_specs=[rows(bq), pl.BlockSpec((kb, 1, bq), lambda ih, iq: (ih, 0, iq))],
        scratch_shapes=[pltpu.VMEM((bq, kb * HEAD), BF), pltpu.VMEM((tokens, kb * HEAD), BF), pltpu.VMEM((kb, HEAD + 8, tokens), BF),
                        pltpu.VMEM((kb, bq), F32), pltpu.VMEM((kb, HEAD + 8, bq), F32), pltpu.VMEM((bq, bq), jnp.int32)],
        out_shape=[jax.ShapeDtypeStruct((tokens, width), BF), jax.ShapeDtypeStruct((heads, 1, tokens), F32)],
        compiler_params=pltpu.CompilerParams(dimension_semantics=("arbitrary", "arbitrary"), vmem_limit_bytes=VMEM),
        cost_estimate=pl.CostEstimate(flops=4 * tokens * tokens * width, transcendentals=heads * tokens * tokens, bytes_accessed=8 * tokens * width),
        name="attend",
    )(q, k, v, cos, sin)


def _backward(q_ref, k_ref, v_ref, do_ref, o_ref, lse_ref, cos_ref, sin_ref, *rest, held, kb, bq, bk, scale):
    d_ref, q_s, k_s, dq_s, dk_s, dv_s, gap_s = rest[held:]
    iq = pl.program_id(1)
    tokens = k_ref.shape[0]
    e = scale * LOG2E

    @pl.when(iq == 0)
    def _():
        gap_s[...] = _gap(bk, bq)
        dk_s[...] = jnp.zeros_like(dk_s)
        dv_s[...] = jnp.zeros_like(dv_s)

        def fill(j, _):
            here = pl.ds(pl.multiple_of(j * 256, 256), 256)
            cos, sin = cos_ref[here, :], sin_ref[here, :]
            for i in range(kb):
                k_s[here, _lanes(i)] = _turn(k_ref[here, _lanes(i)].astype(F32), cos, sin).astype(BF)

        lax.fori_loop(0, tokens // 256, fill, None)

    mine = pl.ds(pl.multiple_of(iq * bq, bq), bq)
    cos, sin = cos_ref[mine, :], sin_ref[mine, :]
    for i in range(kb):
        q_s[:, _lanes(i)] = _turn(q_ref[:, _lanes(i)].astype(F32), cos, sin).astype(BF)
    dq_s[...] = jnp.zeros_like(dq_s)
    lses = [lse_ref[i] * LOG2E for i in range(kb)]
    deltas = [(do_ref[:, _lanes(i)].astype(F32) * o_ref[:, _lanes(i)].astype(F32)).T.sum(axis=0, keepdims=True) for i in range(kb)]

    def block(start, size, first, masked):
        here = pl.ds(pl.multiple_of(start, size), size)
        qs = [q_s[first:, _lanes(i)] for i in range(kb)]
        dos = [do_ref[first:, _lanes(i)] for i in range(kb)]
        scores = [_dot(k_s[here, _lanes(i)], qs[i], 1, 1) for i in range(kb)]
        dps = [_dot(v_ref[here, _lanes(i)], dos[i], 1, 1) for i in range(kb)]
        ok = gap_s[:, : bq - first] >= 0 if masked else None
        for i in range(kb):
            p = jnp.exp2(scores[i] * e - lses[i][:, first:])
            if masked:
                p = jnp.where(ok, p, 0.0)
            ds = (p * (dps[i] - deltas[i][:, first:])).astype(BF)
            dv_s[here, _lanes(i)] += _dot(p.astype(BF), dos[i], 1, 0)
            dk_s[here, _lanes(i)] += _dot(ds, qs[i], 1, 0)
            dq_s[i, :, first:] += _dot(k_s[here, _lanes(i)].T, ds, 1, 0)

    lax.fori_loop(0, iq, lambda j, _: block(j * bq, bq, 0, False), None)
    for first in range(0, bq, bk):
        block(iq * bq + first, bk, first, True)
    for i in range(kb):
        dq = (dq_s[i] * scale).T.astype(BF).astype(F32)
        d_ref[0, mine, _lanes(i)] = _turn(dq, cos, -sin).astype(BF)

    @pl.when(iq == pl.num_programs(1) - 1)
    def _():
        def leave(j, _):
            here = pl.ds(pl.multiple_of(j * 256, 256), 256)
            cos, sin = cos_ref[here, :], sin_ref[here, :]
            for i in range(kb):
                dk = (dk_s[here, _lanes(i)] * scale).astype(BF).astype(F32)
                d_ref[1, here, _lanes(i)] = _turn(dk, cos, -sin).astype(BF)
                d_ref[2, here, _lanes(i)] = dv_s[here, _lanes(i)].astype(BF)

        lax.fori_loop(0, tokens // 256, leave, None)


def attend_bwd(q, k, v, d_out, out, lse, cos, sin, first=0, groups=3, before=None, whole=True, kb=4, bq=512, bk=256):
    tokens, width = q.shape
    heads = groups * kb
    rows = lambda n: pl.BlockSpec((n, kb * HEAD), lambda ih, iq: (iq if n == bq else 0, ih + first))
    table = pl.BlockSpec((tokens, HEAD), lambda ih, iq: (0, 0))
    held = [] if before is None else [before]
    return pl.pallas_call(
        functools.partial(_backward, held=len(held), kb=kb, bq=bq, bk=bk, scale=HEAD**-0.5),
        grid=(groups, tokens // bq),
        in_specs=[rows(bq), rows(tokens), rows(tokens), rows(bq), rows(bq), pl.BlockSpec((kb, 1, bq), lambda ih, iq: (ih + first, 0, iq)), table, table,
                  *[pl.BlockSpec(memory_space=pl.ANY)] * len(held)],
        out_specs=pl.BlockSpec((3, tokens, kb * HEAD), lambda ih, iq: (0, 0, ih + first if whole else ih)),
        scratch_shapes=[pltpu.VMEM((bq, kb * HEAD), BF), pltpu.VMEM((tokens, kb * HEAD), BF), pltpu.VMEM((kb, HEAD, bq), F32),
                        pltpu.VMEM((tokens, kb * HEAD), F32), pltpu.VMEM((tokens, kb * HEAD), F32), pltpu.VMEM((bk, bq), jnp.int32)],
        out_shape=jax.ShapeDtypeStruct((3, tokens, width if whole else heads * HEAD), BF),
        input_output_aliases={8: 0} if held else {},
        compiler_params=pltpu.CompilerParams(dimension_semantics=("arbitrary", "arbitrary"), vmem_limit_bytes=VMEM),
        cost_estimate=pl.CostEstimate(flops=10 * tokens * tokens * heads * HEAD, transcendentals=heads * tokens * tokens, bytes_accessed=16 * tokens * heads * HEAD),
        name="attend_bwd",
    )(q, k, v, d_out, out, lse, cos, sin, *held)


def _mlp(b_ref, wg_ref, wu_ref, gate_ref, up_ref, act_ref, *, tm, ch):
    b = b_ref[pl.ds(pl.multiple_of(pl.program_id(1) * tm, tm), tm), :]
    for at in range(0, act_ref.shape[1], ch):
        here = slice(at, at + ch)
        gate, up = _dot(b, wg_ref[:, here], 1, 0), _dot(b, wu_ref[:, here], 1, 0)
        gate_ref[:, here], up_ref[:, here] = gate, up
        act_ref[:, here] = (gate * jax.nn.sigmoid(gate) * up).astype(BF)


def mlp(b, w_gate, w_up, n, tm=2048, tn=256, ch=256):
    (tokens, d), ff = b.shape, w_gate.shape[2]
    tile = pl.BlockSpec((tm, tn), lambda j, i: (i, j))
    weight = pl.BlockSpec((None, d, tn), lambda j, i: (n, 0, j))
    return pl.pallas_call(
        functools.partial(_mlp, tm=tm, ch=ch),
        grid=(ff // tn, tokens // tm),
        in_specs=[pl.BlockSpec((tokens, d), lambda j, i: (0, 0)), weight, weight],
        out_specs=[tile] * 3,
        out_shape=[jax.ShapeDtypeStruct((tokens, ff), t) for t in (F32, F32, BF)],
        compiler_params=pltpu.CompilerParams(dimension_semantics=("arbitrary", "arbitrary"), vmem_limit_bytes=VMEM),
        cost_estimate=pl.CostEstimate(flops=4 * tokens * d * ff, transcendentals=tokens * ff, bytes_accessed=10 * tokens * ff + 4 * d * ff),
        name="mlp",
    )(b, w_gate, w_up)


def _mlp_bwd(d_ref, w_ref, gate_ref, up_ref, out_ref, *, tm, ch):
    d = d_ref[pl.ds(pl.multiple_of(pl.program_id(1) * tm, tm), tm), :]
    for at in range(0, gate_ref.shape[1], ch):
        here = slice(at, at + ch)
        d_act = _dot(d, w_ref[here, :], 1, 1).astype(BF).astype(F32)
        gate = gate_ref[:, here]
        s = jax.nn.sigmoid(gate)
        out_ref[0, :, here] = (d_act * up_ref[:, here] * (s * (1 + gate * (1 - s)))).astype(BF)
        out_ref[1, :, here] = (d_act * (gate * s)).astype(BF)


def mlp_inner_bwd(d, w_down, gate, up, n, tm=512, tn=1024, ch=256):
    (tokens, width), ff = d.shape, w_down.shape[1]
    tile = pl.BlockSpec((tm, tn), lambda j, i: (i, j))
    return pl.pallas_call(
        functools.partial(_mlp_bwd, tm=tm, ch=ch),
        grid=(ff // tn, tokens // tm),
        in_specs=[pl.BlockSpec((tokens, width), lambda j, i: (0, 0)), pl.BlockSpec((None, tn, width), lambda j, i: (n, j, 0)), tile, tile],
        out_specs=pl.BlockSpec((2, tm, tn), lambda j, i: (0, i, j)),
        out_shape=jax.ShapeDtypeStruct((2, tokens, ff), BF),
        compiler_params=pltpu.CompilerParams(dimension_semantics=("arbitrary", "arbitrary"), vmem_limit_bytes=VMEM),
        cost_estimate=pl.CostEstimate(flops=2 * tokens * width * ff, transcendentals=tokens * ff, bytes_accessed=12 * tokens * ff),
        name="mlp_bwd",
    )(d, w_down, gate, up)


def _grads(*refs, starts):
    out_ref, left_s = refs[-2:]
    s = pl.program_id(0)
    for i, (start, end) in enumerate(zip(starts, starts[1:])):
        a_ref, d_ref = refs[2 * i : 2 * i + 2]

        @pl.when(s == start)
        def _():
            left_s[...] = a_ref[...].T

        @pl.when((s >= start) & (s < end))
        def _():
            out_ref[...] = _dot(left_s[...], d_ref[...], 1, 0).astype(BF)


def grads(*pairs, tn=512):
    tokens, rows = pairs[0][0].shape
    starts, specs = [0], []
    for _, d in pairs:
        parts, _, n = d.shape
        f, start, last = n // tn, starts[-1], parts * (n // tn) - 1
        at = lambda s, start=start, last=last: jnp.clip(s - start, 0, last)
        specs += [pl.BlockSpec((tokens, rows), lambda s: (0, 0)), pl.BlockSpec((None, tokens, tn), lambda s, at=at, f=f: (lax.div(at(s), f), 0, lax.rem(at(s), f)))]
        starts.append(start + last + 1)
    n = starts[-1] * tn
    return pl.pallas_call(
        functools.partial(_grads, starts=tuple(starts)),
        grid=(starts[-1],),
        in_specs=specs,
        out_specs=pl.BlockSpec((rows, tn), lambda s: (0, s)),
        out_shape=jax.ShapeDtypeStruct((rows, n), BF),
        scratch_shapes=[pltpu.VMEM((rows, tokens), BF)],
        compiler_params=pltpu.CompilerParams(dimension_semantics=("arbitrary",), vmem_limit_bytes=VMEM),
        cost_estimate=pl.CostEstimate(flops=2 * tokens * rows * n, transcendentals=0, bytes_accessed=2 * (tokens + rows) * n),
        name="grads",
    )(*[x for pair in pairs for x in pair])


def _update(factor_ref, *refs, pieces):
    count, at = len(pieces), 0
    factor = factor_ref[0:1, 0:1]
    old, new = refs[sum(pieces) :], refs[-3 * count :]
    for i in range(count):
        g = jnp.concatenate([refs[at + j][...] for j in range(pieces[i])], 1) if pieces[i] > 1 else refs[at][...]
        at += pieces[i]
        g = g.astype(F32)
        g = (g.T if i == count - 1 else g) * factor
        w, m, v = (old[3 * i + j][...] for j in range(3))
        m = 0.9 * m + 0.1 * g
        v = 0.95 * v + 0.05 * g * g
        w = w.astype(F32)
        new[3 * i][...] = (w - 0.02 * (m * lax.rsqrt(v + 1e-8) + 0.1 * w)).astype(BF)
        new[3 * i + 1][...] = m
        new[3 * i + 2][...] = v


def update(factor, gs, state, n, before, cut):
    count, (down, across) = len(gs), cut
    steps = down * across
    specs, blocks = [], []
    for i, pieces in enumerate(gs):
        _, r, c = state[3 * i].shape
        if i < count - 1:
            blocks += [pl.BlockSpec((None, r // steps, c), lambda s: (n, s, 0))] * 3
            specs += [pl.BlockSpec((r // steps, wide), lambda s, at=at // wide: (s, at)) for _, at, wide in pieces]
        else:
            blocks += [pl.BlockSpec((None, r // down, c // across), lambda s: (n, lax.div(s, across), lax.rem(s, across)))] * 3
            specs += [pl.BlockSpec((c // across, r // down), lambda s, at=at // (r // down): (lax.rem(s, across), at + lax.div(s, across))) for _, at, _ in pieces]
    held = [] if before is None else list(before)
    size = sum(x.size // x.shape[0] for x in state[::3])
    return pl.pallas_call(
        functools.partial(_update, pieces=tuple(len(p) for p in gs)),
        grid=(steps,),
        in_specs=[pl.BlockSpec((8, 128), lambda s: (0, 0)), *specs, *blocks, *[pl.BlockSpec(memory_space=pl.ANY)] * len(held)],
        out_specs=blocks,
        out_shape=[jax.ShapeDtypeStruct(x.shape, x.dtype) for x in state],
        input_output_aliases={1 + len(specs) + len(state) + j: j for j in range(len(held))},
        compiler_params=pltpu.CompilerParams(dimension_semantics=("arbitrary",), vmem_limit_bytes=VMEM),
        cost_estimate=pl.CostEstimate(flops=15 * size, transcendentals=size, bytes_accessed=22 * size),
        name="update",
    )(factor, *[g for pieces in gs for g, _, _ in pieces], *state, *held)


def _back(d_ref, *refs, parts, per):
    w_refs, (h_ref, by_ref, out_ref, sum_s) = refs[:parts], refs[parts:]
    s = pl.program_id(0)
    for p in range(parts):
        @pl.when(lax.div(s, per) == p)
        def _():
            got = _dot(d_ref[...], w_refs[p][...], 1, 1)
            if p == 0:
                @pl.when(s == 0)
                def _():
                    sum_s[...] = got

                @pl.when(s > 0)
                def _():
                    sum_s[...] += got
            else:
                sum_s[...] += got

    @pl.when(s == pl.num_programs(0) - 1)
    def _():
        def rows(j, _):
            here = pl.ds(pl.multiple_of(j * 256, 256), 256)
            wide, d = h_ref[here, :].astype(F32), sum_s[here, :].astype(BF).astype(F32)
            scale = lax.rsqrt(jnp.mean(wide * wide, -1, keepdims=True) + 1e-6)
            unit = wide * scale
            d = (scale * (d - unit * jnp.mean(d * unit, -1, keepdims=True))).astype(BF)
            out_ref[here, :] = (by_ref[here, :].astype(F32) + d.astype(F32)).astype(BF)

        lax.fori_loop(0, out_ref.shape[0] // 256, rows, None)


def back(d, ws, n, h, by, tk):
    parts, tokens, width = d.shape
    rows = ws[0].shape[1]
    per = width // tk
    whole = pl.BlockSpec((tokens, rows), lambda s: (0, 0))
    weight = lambda p: pl.BlockSpec((None, rows, tk), lambda s: (n, 0, jnp.clip(s - p * per, 0, per - 1)))
    return pl.pallas_call(
        functools.partial(_back, parts=parts, per=per),
        grid=(parts * per,),
        in_specs=[pl.BlockSpec((None, tokens, tk), lambda s: (lax.div(s, per), 0, lax.rem(s, per))), *[weight(p) for p in range(parts)], whole, whole],
        out_specs=whole,
        out_shape=jax.ShapeDtypeStruct((tokens, rows), BF),
        scratch_shapes=[pltpu.VMEM((tokens, rows), F32)],
        compiler_params=pltpu.CompilerParams(dimension_semantics=("arbitrary",), vmem_limit_bytes=VMEM),
        cost_estimate=pl.CostEstimate(flops=2 * tokens * rows * parts * width, transcendentals=tokens, bytes_accessed=2 * (tokens + rows) * parts * width),
        name="back",
    )(d, *ws, h, by)


def _factor(*refs, size):
    shards, (out_ref, mine, got, send, recv) = refs[:-5], refs[-5:]
    n = got.shape[0]
    me = lax.axis_index("dp")
    others = [lax.rem(me + k, n) for k in range(1, n)]
    barrier = pltpu.get_barrier_semaphore()
    for other in others:
        pl.semaphore_signal(barrier, inc=1, device_id={"dp": other}, device_id_type=pl.DeviceIdType.MESH)
    total = jnp.zeros((1, 1), F32)
    for ref in shards:
        wide = 1536 if ref.shape[1] % 1536 == 0 else 1024
        for at in range(0, ref.shape[1], wide):
            def rows(j, so_far):
                x = ref[pl.ds(pl.multiple_of(j * 16, 16), 16), at : at + wide].astype(F32)
                return so_far + x * x

            part = lax.fori_loop(0, ref.shape[0] // 16, rows, jnp.zeros((16, wide), F32))
            total += jnp.sum(jnp.sum(part, axis=0, keepdims=True), axis=1, keepdims=True)
    total = jnp.broadcast_to(total, (8, 128))
    mine[...] = total
    got[me] = total
    pl.semaphore_wait(barrier, n - 1)
    copies = [pltpu.make_async_remote_copy(mine, got.at[me], send.at[k], recv.at[k], device_id={"dp": other}, device_id_type=pl.DeviceIdType.MESH)
              for k, other in enumerate(others)]
    for copy in copies:
        copy.start()
    for k, copy in enumerate(copies):
        copy.wait_send()
        source = lax.rem(me + n - 1 - k, n)
        pltpu.make_async_remote_copy(mine, got.at[source], send.at[k], recv.at[k], device_id={"dp": source}, device_id_type=pl.DeviceIdType.MESH).wait_recv()
    total = got[0]
    for i in range(1, n):
        total += got[i]
    out_ref[...] = jnp.minimum(1.0, 0.5 * lax.rsqrt(total / size + 1e-30))


def clip_factor(shards, n, size):
    return pl.pallas_call(
        functools.partial(_factor, size=size),
        in_specs=[pl.BlockSpec(memory_space=pltpu.VMEM)] * len(shards),
        out_specs=pl.BlockSpec(memory_space=pltpu.VMEM),
        out_shape=jax.ShapeDtypeStruct((8, 128), F32),
        scratch_shapes=[pltpu.VMEM((8, 128), F32), pltpu.VMEM((n, 8, 128), F32), pltpu.SemaphoreType.DMA((n - 1,)), pltpu.SemaphoreType.DMA((n - 1,))],
        compiler_params=pltpu.CompilerParams(collective_id=1, has_side_effects=True, vmem_limit_bytes=VMEM),
        cost_estimate=pl.CostEstimate(flops=2 * size // n, transcendentals=0, bytes_accessed=2 * size // n),
        name="clip_factor",
    )(*shards)


def matmul(a, w):
    return jnp.dot(a, w, preferred_element_type=F32).astype(BF)


def by_left(d, w):
    return _dot(d, w, 1, 1).astype(BF)


def normed(h):
    wide = h.astype(F32)
    scale = lax.rsqrt(jnp.mean(wide**2, -1, keepdims=True) + 1e-6)
    return (wide * scale).astype(BF)


def tables(tokens):
    half = HEAD // 2
    angle = jnp.arange(tokens, dtype=F32)[:, None] * THETA ** (-jnp.arange(half, dtype=F32) / half)
    cos, sin = jnp.cos(angle), jnp.sin(angle)
    return jnp.concatenate([cos, cos], -1), jnp.concatenate([-sin, sin], -1)


def layer(h, w, whole, n, cos, sin):
    a = normed(h)
    q, k, v = (matmul(a, w[name]) for name in ("wq", "wk", "wv"))
    out, lse = attend(q, k, v, cos, sin)
    mid = h + matmul(out, w["wo"])
    b = normed(mid)
    gate, up, act = mlp(b, whole["w_gate"], whole["w_up"], n)
    return mid + matmul(act, w["w_down"]), (h, a, q, k, v, out, lse, mid, b, gate, up, act)


MLP, ATTENTION = ("w_gate", "w_up", "w_down"), ("wq", "wk", "wv", "wo")


def solution(mesh):
    tie = lax.optimization_barrier

    def scatter(g):
        return lax.psum_scatter(g, "dp", scatter_dimension=0, tiled=True)

    def gather(g):
        return lax.all_gather(g, "dp", axis=0, tiled=True)

    def step(x, dy, *arrays):
        weights, m, v = (dict(zip(NAMES, arrays[i : i + 7], strict=True)) for i in (0, 7, 14))
        count = weights["wq"].shape[0]
        layers = [{name: w[n] for name, w in weights.items()} for n in range(count)]
        cos, sin = tables(x.shape[1])
        h, kept = x[0], []
        for n, w in enumerate(layers):
            h, some = layer(h, w, weights, n, cos, sin)
            kept.append(some)
        d = dy[0]
        width, ff = weights["wq"].shape[2], weights["w_gate"].shape[2]
        cut = 8 * HEAD
        shards, full, gs = {}, {}, {}

        def send(n, tag, g, places):
            shards[n, tag] = scatter(g)
            at = 0
            for name, wide in places:
                gs.setdefault((n, name), []).append(((n, tag), at, wide))
                at += wide

        for n in reversed(range(count)):
            h, a, q, k, values, out, lse, mid, b, gate, up, act = kept[n]
            last = n == count - 1
            if last:
                d, g = tie((d, grads((d, act[None]))))
                send(n, "down", g, [("w_down", ff)])
            d_gu = mlp_inner_bwd(d, weights["w_down"], gate, up, n)
            d_gu, g = tie((d_gu, grads((b, d_gu)) if last else grads((b, d_gu), (d, act[None]))))
            send(n, "mlp", g, [("w_gate", ff), ("w_up", ff)] + [("w_down", ff)] * (not last))
            d_mid = back(d_gu, (weights["w_gate"], weights["w_up"]), n, mid, d, 1024)
            if not last:
                d_mid, full[n + 1, "down"], full[n + 1, "mlp"] = tie((d_mid, full[n + 1, "down"], full[n + 1, "mlp"]))
            args = (q, k, values, by_left(d_mid, layers[n]["wo"]), out, lse, cos, sin)
            d = attend_bwd(*args, first=0, groups=2, whole=n > 0)
            if n > 0:
                d, shards[n, "down"], shards[n, "mlp"] = tie((d, shards[n, "down"], shards[n, "mlp"]))
                full[n, "down"], full[n, "mlp"] = gather(shards[n, "down"]), gather(shards[n, "mlp"])
                d = attend_bwd(*args, first=2, groups=1, before=d)
                d, g = tie((d, grads((a, d), (d_mid, out[None]))))
                send(n, "attention", g, [("wq", width), ("wk", width), ("wv", width), ("wo", width)])
                d = back(d, tuple(weights[name] for name in ("wq", "wk", "wv")), n, h, d_mid, 768)
            else:
                args, g, shards[n + 1, "attention"] = tie((args, grads((a, d), (d_mid, out[None])), shards[n + 1, "attention"]))
                send(n, "early", g, [("wq", cut), ("wk", cut), ("wv", cut), ("wo", width)])
                d = attend_bwd(*args, first=2, groups=1, whole=False)
                d, shards[n, "mlp"] = tie((d, shards[n, "mlp"]))
                g, shards[n, "early"] = tie((grads((a, d)), shards[n, "early"]))
                send(n, "late", g, [("wq", width - cut), ("wk", width - cut), ("wv", width - cut)])
        shards = dict(zip(shards, tie(tuple(shards.values()))))
        factor = clip_factor(tuple(shards.values()), mesh.shape["dp"], sum(w.size for w in weights.values()))
        got = {MLP: None, ATTENTION: None}
        for part, blocks in ((MLP, (16, 1)), (ATTENTION, (4, 4))):
            state = [of[name] for name in part for of in (weights, m, v)]
            for n in reversed(range(count)):
                for name in part:
                    for key, _, _ in gs[n, name]:
                        if key not in full:
                            full[key] = gather(shards[key])
                pieces = [[(full[key], at, wide) for key, at, wide in gs[n, name]] for name in part]
                got[part] = update(factor, pieces, state, n, got[part], blocks)
                factor, got[part] = tie((factor, got[part]))
        new = {name: got[part][3 * i : 3 * i + 3] for part in got for i, name in enumerate(part)}
        return tuple(new[name][which] for which in range(3) for name in NAMES)

    states, all_of = P(("rep", "dp"), None, None), P(None, None, None)
    return jax.shard_map(
        step,
        mesh=mesh,
        in_specs=(states, states) + (all_of,) * 21,
        out_specs=(P("rep", None, None),) * 21,
        check_vma=False,
    )
```

```python
import functools

import jax
import jax.numpy as jnp
from jax import lax
from jax.experimental import pallas as pl
from jax.experimental.pallas import tpu as pltpu
from jax.sharding import PartitionSpec as P

NEG = -1e30
HIDDEN = 2 * NEG
LOG2E = 1.4426950408889634
VMEM = 58 * 2**20
HEAD = 128
THETA = 10000
NAMES = ("wq", "wk", "wv", "wo", "w_gate", "w_up", "w_down")
BF = jnp.bfloat16
F32 = jnp.float32


def _dot(a, b, ca, cb):
    return lax.dot_general(a, b, (((ca,), (cb,)), ((), ())), preferred_element_type=F32)


def _turn(x, cos, sin):
    return x * cos + pltpu.roll(x, HEAD // 2, 1) * sin


def _gap(bk, bq):
    return lax.broadcasted_iota(jnp.int32, (bk, bq), 1) - lax.broadcasted_iota(jnp.int32, (bk, bq), 0)


def _lanes(i):
    return slice(i * HEAD, (i + 1) * HEAD)


def _forward(q_ref, k_ref, v_ref, cos_ref, sin_ref, o_ref, lse_ref, q_s, k_s, v_s, top_s, mix_s, gap_s, *, kb, bq, bk, scale):
    iq = pl.program_id(1)
    tokens = k_ref.shape[0]
    e = scale * LOG2E

    @pl.when(iq == 0)
    def _():
        gap_s[...] = _gap(bq, bq)

        def fill(j, _):
            here = pl.ds(pl.multiple_of(j * 256, 256), 256)
            cos, sin = cos_ref[here, :], sin_ref[here, :]
            for i in range(kb):
                k_s[here, _lanes(i)] = _turn(k_ref[here, _lanes(i)].astype(F32), cos, sin).astype(BF)
                v_s[i, :HEAD, here] = v_ref[here, _lanes(i)].T
                v_s[i, HEAD:, here] = jnp.ones((8, 256), BF)

        lax.fori_loop(0, tokens // 256, fill, None)

    mine = pl.ds(pl.multiple_of(iq * bq, bq), bq)
    cos, sin = cos_ref[mine, :], sin_ref[mine, :]
    for i in range(kb):
        q_s[:, _lanes(i)] = _turn(q_ref[:, _lanes(i)].astype(F32), cos, sin).astype(BF)
    top_s[...] = jnp.full(top_s.shape, NEG, F32)
    mix_s[...] = jnp.zeros(mix_s.shape, F32)

    def block(start, size, masked):
        here = pl.ds(pl.multiple_of(start, size), size)
        scores = [_dot(k_s[here, _lanes(i)], q_s[:, _lanes(i)], 1, 1) for i in range(kb)]
        ok = gap_s[...] >= 0 if masked else None
        weights, keeps = [], []
        for i, s in enumerate(scores):
            if masked:
                s = jnp.where(ok, s, HIDDEN)
            old = top_s[i : i + 1, :]
            top = jnp.maximum(old, s.max(axis=0, keepdims=True))
            top_s[i : i + 1, :] = top
            weights.append(jnp.exp2((s - top) * e).astype(BF))
            keeps.append(jnp.exp2((old - top) * e))
        for i, (p, keep) in enumerate(zip(weights, keeps)):
            mix_s[i] = mix_s[i] * keep + _dot(v_s[i, :, here], p, 1, 0)

    whole = lax.div(iq * bq, bk)
    lax.fori_loop(0, whole, lambda j, _: block(j * bk, bk, False), None)
    lax.fori_loop(whole * (bk // bq), iq, lambda j, _: block(j * bq, bq, False), None)
    block(iq * bq, bq, True)
    for i in range(kb):
        top, total = top_s[i : i + 1, :], mix_s[i, HEAD : HEAD + 1, :]
        o_ref[:, _lanes(i)] = (mix_s[i, :HEAD, :] * (1 / total)).T.astype(BF)
        lse_ref[i] = top * scale + jnp.log(total)


def attend(q, k, v, cos, sin, kb=12, bq=256, bk=512):
    tokens, width = q.shape
    heads = width // HEAD
    rows = lambda n: pl.BlockSpec((n, kb * HEAD), lambda ih, iq: (iq if n == bq else 0, ih))
    table = pl.BlockSpec((tokens, HEAD), lambda ih, iq: (0, 0))
    return pl.pallas_call(
        functools.partial(_forward, kb=kb, bq=bq, bk=bk, scale=HEAD**-0.5),
        grid=(heads // kb, tokens // bq),
        in_specs=[rows(bq), rows(tokens), rows(tokens), table, table],
        out_specs=[rows(bq), pl.BlockSpec((kb, 1, bq), lambda ih, iq: (ih, 0, iq))],
        scratch_shapes=[pltpu.VMEM((bq, kb * HEAD), BF), pltpu.VMEM((tokens, kb * HEAD), BF), pltpu.VMEM((kb, HEAD + 8, tokens), BF),
                        pltpu.VMEM((kb, bq), F32), pltpu.VMEM((kb, HEAD + 8, bq), F32), pltpu.VMEM((bq, bq), jnp.int32)],
        out_shape=[jax.ShapeDtypeStruct((tokens, width), BF), jax.ShapeDtypeStruct((heads, 1, tokens), F32)],
        compiler_params=pltpu.CompilerParams(dimension_semantics=("arbitrary", "arbitrary"), vmem_limit_bytes=VMEM),
        cost_estimate=pl.CostEstimate(flops=4 * tokens * tokens * width, transcendentals=heads * tokens * tokens, bytes_accessed=8 * tokens * width),
        name="attend",
    )(q, k, v, cos, sin)


def _backward(q_ref, k_ref, v_ref, do_ref, o_ref, lse_ref, cos_ref, sin_ref, *rest, held, kb, bq, bk, scale):
    d_ref, q_s, k_s, dq_s, dk_s, dv_s, gap_s = rest[held:]
    iq = pl.program_id(1)
    tokens = k_ref.shape[0]
    e = scale * LOG2E

    @pl.when(iq == 0)
    def _():
        gap_s[...] = _gap(bk, bq)
        dk_s[...] = jnp.zeros_like(dk_s)
        dv_s[...] = jnp.zeros_like(dv_s)

        def fill(j, _):
            here = pl.ds(pl.multiple_of(j * 256, 256), 256)
            cos, sin = cos_ref[here, :], sin_ref[here, :]
            for i in range(kb):
                k_s[here, _lanes(i)] = _turn(k_ref[here, _lanes(i)].astype(F32), cos, sin).astype(BF)

        lax.fori_loop(0, tokens // 256, fill, None)

    mine = pl.ds(pl.multiple_of(iq * bq, bq), bq)
    cos, sin = cos_ref[mine, :], sin_ref[mine, :]
    for i in range(kb):
        q_s[:, _lanes(i)] = _turn(q_ref[:, _lanes(i)].astype(F32), cos, sin).astype(BF)
    dq_s[...] = jnp.zeros_like(dq_s)
    lses = [lse_ref[i] * LOG2E for i in range(kb)]
    deltas = [(do_ref[:, _lanes(i)].astype(F32) * o_ref[:, _lanes(i)].astype(F32)).T.sum(axis=0, keepdims=True) for i in range(kb)]

    def block(start, size, first, masked):
        here = pl.ds(pl.multiple_of(start, size), size)
        qs = [q_s[first:, _lanes(i)] for i in range(kb)]
        dos = [do_ref[first:, _lanes(i)] for i in range(kb)]
        scores = [_dot(k_s[here, _lanes(i)], qs[i], 1, 1) for i in range(kb)]
        dps = [_dot(v_ref[here, _lanes(i)], dos[i], 1, 1) for i in range(kb)]
        ok = gap_s[:, : bq - first] >= 0 if masked else None
        for i in range(kb):
            p = jnp.exp2(scores[i] * e - lses[i][:, first:])
            if masked:
                p = jnp.where(ok, p, 0.0)
            ds = (p * (dps[i] - deltas[i][:, first:])).astype(BF)
            dv_s[here, _lanes(i)] += _dot(p.astype(BF), dos[i], 1, 0)
            dk_s[here, _lanes(i)] += _dot(ds, qs[i], 1, 0)
            dq_s[i, :, first:] += _dot(k_s[here, _lanes(i)].T, ds, 1, 0)

    lax.fori_loop(0, iq, lambda j, _: block(j * bq, bq, 0, False), None)
    for first in range(0, bq, bk):
        block(iq * bq + first, bk, first, True)
    for i in range(kb):
        dq = (dq_s[i] * scale).T.astype(BF).astype(F32)
        d_ref[0, mine, _lanes(i)] = _turn(dq, cos, -sin).astype(BF)

    @pl.when(iq == pl.num_programs(1) - 1)
    def _():
        def leave(j, _):
            here = pl.ds(pl.multiple_of(j * 256, 256), 256)
            cos, sin = cos_ref[here, :], sin_ref[here, :]
            for i in range(kb):
                dk = (dk_s[here, _lanes(i)] * scale).astype(BF).astype(F32)
                d_ref[1, here, _lanes(i)] = _turn(dk, cos, -sin).astype(BF)
                d_ref[2, here, _lanes(i)] = dv_s[here, _lanes(i)].astype(BF)

        lax.fori_loop(0, tokens // 256, leave, None)


def attend_bwd(q, k, v, d_out, out, lse, cos, sin, first=0, groups=3, before=None, whole=True, kb=4, bq=512, bk=256):
    tokens, width = q.shape
    heads = groups * kb
    rows = lambda n: pl.BlockSpec((n, kb * HEAD), lambda ih, iq: (iq if n == bq else 0, ih + first))
    table = pl.BlockSpec((tokens, HEAD), lambda ih, iq: (0, 0))
    held = [] if before is None else [before]
    return pl.pallas_call(
        functools.partial(_backward, held=len(held), kb=kb, bq=bq, bk=bk, scale=HEAD**-0.5),
        grid=(groups, tokens // bq),
        in_specs=[rows(bq), rows(tokens), rows(tokens), rows(bq), rows(bq), pl.BlockSpec((kb, 1, bq), lambda ih, iq: (ih + first, 0, iq)), table, table,
                  *[pl.BlockSpec(memory_space=pl.ANY)] * len(held)],
        out_specs=pl.BlockSpec((3, tokens, kb * HEAD), lambda ih, iq: (0, 0, ih + first if whole else ih)),
        scratch_shapes=[pltpu.VMEM((bq, kb * HEAD), BF), pltpu.VMEM((tokens, kb * HEAD), BF), pltpu.VMEM((kb, HEAD, bq), F32),
                        pltpu.VMEM((tokens, kb * HEAD), F32), pltpu.VMEM((tokens, kb * HEAD), F32), pltpu.VMEM((bk, bq), jnp.int32)],
        out_shape=jax.ShapeDtypeStruct((3, tokens, width if whole else heads * HEAD), BF),
        input_output_aliases={8: 0} if held else {},
        compiler_params=pltpu.CompilerParams(dimension_semantics=("arbitrary", "arbitrary"), vmem_limit_bytes=VMEM),
        cost_estimate=pl.CostEstimate(flops=10 * tokens * tokens * heads * HEAD, transcendentals=heads * tokens * tokens, bytes_accessed=16 * tokens * heads * HEAD),
        name="attend_bwd",
    )(q, k, v, d_out, out, lse, cos, sin, *held)


def _mlp(b_ref, wg_ref, wu_ref, gate_ref, up_ref, act_ref, *, tm, ch):
    b = b_ref[pl.ds(pl.multiple_of(pl.program_id(1) * tm, tm), tm), :]
    for at in range(0, act_ref.shape[1], ch):
        here = slice(at, at + ch)
        gate, up = _dot(b, wg_ref[:, here], 1, 0), _dot(b, wu_ref[:, here], 1, 0)
        gate_ref[:, here], up_ref[:, here] = gate, up
        act_ref[:, here] = (gate * jax.nn.sigmoid(gate) * up).astype(BF)


def mlp(b, w_gate, w_up, n, tm=2048, tn=256, ch=256):
    (tokens, d), ff = b.shape, w_gate.shape[2]
    tile = pl.BlockSpec((tm, tn), lambda j, i: (i, j))
    weight = pl.BlockSpec((None, d, tn), lambda j, i: (n, 0, j))
    return pl.pallas_call(
        functools.partial(_mlp, tm=tm, ch=ch),
        grid=(ff // tn, tokens // tm),
        in_specs=[pl.BlockSpec((tokens, d), lambda j, i: (0, 0)), weight, weight],
        out_specs=[tile] * 3,
        out_shape=[jax.ShapeDtypeStruct((tokens, ff), t) for t in (F32, F32, BF)],
        compiler_params=pltpu.CompilerParams(dimension_semantics=("arbitrary", "arbitrary"), vmem_limit_bytes=VMEM),
        cost_estimate=pl.CostEstimate(flops=4 * tokens * d * ff, transcendentals=tokens * ff, bytes_accessed=10 * tokens * ff + 4 * d * ff),
        name="mlp",
    )(b, w_gate, w_up)


def _mlp_bwd(d_ref, w_ref, gate_ref, up_ref, out_ref, *, tm, ch):
    d = d_ref[pl.ds(pl.multiple_of(pl.program_id(1) * tm, tm), tm), :]
    for at in range(0, gate_ref.shape[1], ch):
        here = slice(at, at + ch)
        d_act = _dot(d, w_ref[here, :], 1, 1).astype(BF).astype(F32)
        gate = gate_ref[:, here]
        s = jax.nn.sigmoid(gate)
        out_ref[0, :, here] = (d_act * up_ref[:, here] * (s * (1 + gate * (1 - s)))).astype(BF)
        out_ref[1, :, here] = (d_act * (gate * s)).astype(BF)


def mlp_inner_bwd(d, w_down, gate, up, n, tm=512, tn=1024, ch=256):
    (tokens, width), ff = d.shape, w_down.shape[1]
    tile = pl.BlockSpec((tm, tn), lambda j, i: (i, j))
    return pl.pallas_call(
        functools.partial(_mlp_bwd, tm=tm, ch=ch),
        grid=(ff // tn, tokens // tm),
        in_specs=[pl.BlockSpec((tokens, width), lambda j, i: (0, 0)), pl.BlockSpec((None, tn, width), lambda j, i: (n, j, 0)), tile, tile],
        out_specs=pl.BlockSpec((2, tm, tn), lambda j, i: (0, i, j)),
        out_shape=jax.ShapeDtypeStruct((2, tokens, ff), BF),
        compiler_params=pltpu.CompilerParams(dimension_semantics=("arbitrary", "arbitrary"), vmem_limit_bytes=VMEM),
        cost_estimate=pl.CostEstimate(flops=2 * tokens * width * ff, transcendentals=tokens * ff, bytes_accessed=12 * tokens * ff),
        name="mlp_bwd",
    )(d, w_down, gate, up)


def _grads(*refs, starts):
    out_ref, left_s = refs[-2:]
    s = pl.program_id(0)
    for i, (start, end) in enumerate(zip(starts, starts[1:])):
        a_ref, d_ref = refs[2 * i : 2 * i + 2]

        @pl.when(s == start)
        def _():
            left_s[...] = a_ref[...].T

        @pl.when((s >= start) & (s < end))
        def _():
            out_ref[...] = _dot(left_s[...], d_ref[...], 1, 0).astype(BF)


def grads(*pairs, tn=512):
    tokens, rows = pairs[0][0].shape
    starts, specs = [0], []
    for _, d in pairs:
        parts, _, n = d.shape
        f, start, last = n // tn, starts[-1], parts * (n // tn) - 1
        at = lambda s, start=start, last=last: jnp.clip(s - start, 0, last)
        specs += [pl.BlockSpec((tokens, rows), lambda s: (0, 0)), pl.BlockSpec((None, tokens, tn), lambda s, at=at, f=f: (lax.div(at(s), f), 0, lax.rem(at(s), f)))]
        starts.append(start + last + 1)
    n = starts[-1] * tn
    return pl.pallas_call(
        functools.partial(_grads, starts=tuple(starts)),
        grid=(starts[-1],),
        in_specs=specs,
        out_specs=pl.BlockSpec((rows, tn), lambda s: (0, s)),
        out_shape=jax.ShapeDtypeStruct((rows, n), BF),
        scratch_shapes=[pltpu.VMEM((rows, tokens), BF)],
        compiler_params=pltpu.CompilerParams(dimension_semantics=("arbitrary",), vmem_limit_bytes=VMEM),
        cost_estimate=pl.CostEstimate(flops=2 * tokens * rows * n, transcendentals=0, bytes_accessed=2 * (tokens + rows) * n),
        name="grads",
    )(*[x for pair in pairs for x in pair])


def _update(factor_ref, *refs, pieces):
    count, at = len(pieces), 0
    factor = factor_ref[0:1, 0:1]
    old, new = refs[sum(pieces) :], refs[-3 * count :]
    for i in range(count):
        g = jnp.concatenate([refs[at + j][...] for j in range(pieces[i])], 1) if pieces[i] > 1 else refs[at][...]
        at += pieces[i]
        g = g.astype(F32)
        g = (g.T if i == count - 1 else g) * factor
        w, m, v = (old[3 * i + j][...] for j in range(3))
        m = 0.9 * m + 0.1 * g
        v = 0.95 * v + 0.05 * g * g
        w = w.astype(F32)
        new[3 * i][...] = (w - 0.02 * (m * lax.rsqrt(v + 1e-8) + 0.1 * w)).astype(BF)
        new[3 * i + 1][...] = m
        new[3 * i + 2][...] = v


def update(factor, gs, state, n, before, cut):
    count, (down, across) = len(gs), cut
    steps = down * across
    specs, blocks = [], []
    for i, pieces in enumerate(gs):
        _, r, c = state[3 * i].shape
        if i < count - 1:
            blocks += [pl.BlockSpec((None, r // steps, c), lambda s: (n, s, 0))] * 3
            specs += [pl.BlockSpec((r // steps, wide), lambda s, at=at // wide: (s, at)) for _, at, wide in pieces]
        else:
            blocks += [pl.BlockSpec((None, r // down, c // across), lambda s: (n, lax.div(s, across), lax.rem(s, across)))] * 3
            specs += [pl.BlockSpec((c // across, r // down), lambda s, at=at // (r // down): (lax.rem(s, across), at + lax.div(s, across))) for _, at, _ in pieces]
    held = [] if before is None else list(before)
    size = sum(x.size // x.shape[0] for x in state[::3])
    return pl.pallas_call(
        functools.partial(_update, pieces=tuple(len(p) for p in gs)),
        grid=(steps,),
        in_specs=[pl.BlockSpec((8, 128), lambda s: (0, 0)), *specs, *blocks, *[pl.BlockSpec(memory_space=pl.ANY)] * len(held)],
        out_specs=blocks,
        out_shape=[jax.ShapeDtypeStruct(x.shape, x.dtype) for x in state],
        input_output_aliases={1 + len(specs) + len(state) + j: j for j in range(len(held))},
        compiler_params=pltpu.CompilerParams(dimension_semantics=("arbitrary",), vmem_limit_bytes=VMEM),
        cost_estimate=pl.CostEstimate(flops=15 * size, transcendentals=size, bytes_accessed=22 * size),
        name="update",
    )(factor, *[g for pieces in gs for g, _, _ in pieces], *state, *held)


def _back(d_ref, *refs, parts, per):
    w_refs, (h_ref, by_ref, out_ref, sum_s) = refs[:parts], refs[parts:]
    s = pl.program_id(0)
    for p in range(parts):
        @pl.when(lax.div(s, per) == p)
        def _():
            got = _dot(d_ref[...], w_refs[p][...], 1, 1)
            if p == 0:
                @pl.when(s == 0)
                def _():
                    sum_s[...] = got

                @pl.when(s > 0)
                def _():
                    sum_s[...] += got
            else:
                sum_s[...] += got

    @pl.when(s == pl.num_programs(0) - 1)
    def _():
        def rows(j, _):
            here = pl.ds(pl.multiple_of(j * 256, 256), 256)
            wide, d = h_ref[here, :].astype(F32), sum_s[here, :].astype(BF).astype(F32)
            scale = lax.rsqrt(jnp.mean(wide * wide, -1, keepdims=True) + 1e-6)
            unit = wide * scale
            d = (scale * (d - unit * jnp.mean(d * unit, -1, keepdims=True))).astype(BF)
            out_ref[here, :] = (by_ref[here, :].astype(F32) + d.astype(F32)).astype(BF)

        lax.fori_loop(0, out_ref.shape[0] // 256, rows, None)


def back(d, ws, n, h, by, tk):
    parts, tokens, width = d.shape
    rows = ws[0].shape[1]
    per = width // tk
    whole = pl.BlockSpec((tokens, rows), lambda s: (0, 0))
    weight = lambda p: pl.BlockSpec((None, rows, tk), lambda s: (n, 0, jnp.clip(s - p * per, 0, per - 1)))
    return pl.pallas_call(
        functools.partial(_back, parts=parts, per=per),
        grid=(parts * per,),
        in_specs=[pl.BlockSpec((None, tokens, tk), lambda s: (lax.div(s, per), 0, lax.rem(s, per))), *[weight(p) for p in range(parts)], whole, whole],
        out_specs=whole,
        out_shape=jax.ShapeDtypeStruct((tokens, rows), BF),
        scratch_shapes=[pltpu.VMEM((tokens, rows), F32)],
        compiler_params=pltpu.CompilerParams(dimension_semantics=("arbitrary",), vmem_limit_bytes=VMEM),
        cost_estimate=pl.CostEstimate(flops=2 * tokens * rows * parts * width, transcendentals=tokens, bytes_accessed=2 * (tokens + rows) * parts * width),
        name="back",
    )(d, *ws, h, by)


def _factor(*refs, size):
    shards, (out_ref, mine, got, send, recv) = refs[:-5], refs[-5:]
    n = got.shape[0]
    me = lax.axis_index("dp")
    others = [lax.rem(me + k, n) for k in range(1, n)]
    barrier = pltpu.get_barrier_semaphore()
    for other in others:
        pl.semaphore_signal(barrier, inc=1, device_id={"dp": other}, device_id_type=pl.DeviceIdType.MESH)
    total = jnp.zeros((1, 1), F32)
    for ref in shards:
        wide = 1536 if ref.shape[1] % 1536 == 0 else 1024
        for at in range(0, ref.shape[1], wide):
            def rows(j, so_far):
                x = ref[pl.ds(pl.multiple_of(j * 16, 16), 16), at : at + wide].astype(F32)
                return so_far + x * x

            part = lax.fori_loop(0, ref.shape[0] // 16, rows, jnp.zeros((16, wide), F32))
            total += jnp.sum(jnp.sum(part, axis=0, keepdims=True), axis=1, keepdims=True)
    total = jnp.broadcast_to(total, (8, 128))
    mine[...] = total
    got[me] = total
    pl.semaphore_wait(barrier, n - 1)
    copies = [pltpu.make_async_remote_copy(mine, got.at[me], send.at[k], recv.at[k], device_id={"dp": other}, device_id_type=pl.DeviceIdType.MESH)
              for k, other in enumerate(others)]
    for copy in copies:
        copy.start()
    for k, copy in enumerate(copies):
        copy.wait_send()
        source = lax.rem(me + n - 1 - k, n)
        pltpu.make_async_remote_copy(mine, got.at[source], send.at[k], recv.at[k], device_id={"dp": source}, device_id_type=pl.DeviceIdType.MESH).wait_recv()
    total = got[0]
    for i in range(1, n):
        total += got[i]
    out_ref[...] = jnp.minimum(1.0, 0.5 * lax.rsqrt(total / size + 1e-30))


def clip_factor(shards, n, size):
    return pl.pallas_call(
        functools.partial(_factor, size=size),
        in_specs=[pl.BlockSpec(memory_space=pltpu.VMEM)] * len(shards),
        out_specs=pl.BlockSpec(memory_space=pltpu.VMEM),
        out_shape=jax.ShapeDtypeStruct((8, 128), F32),
        scratch_shapes=[pltpu.VMEM((8, 128), F32), pltpu.VMEM((n, 8, 128), F32), pltpu.SemaphoreType.DMA((n - 1,)), pltpu.SemaphoreType.DMA((n - 1,))],
        compiler_params=pltpu.CompilerParams(collective_id=1, has_side_effects=True, vmem_limit_bytes=VMEM),
        cost_estimate=pl.CostEstimate(flops=2 * size // n, transcendentals=0, bytes_accessed=2 * size // n),
        name="clip_factor",
    )(*shards)


def matmul(a, w):
    return jnp.dot(a, w, preferred_element_type=F32).astype(BF)


def by_left(d, w):
    return _dot(d, w, 1, 1).astype(BF)


def normed(h):
    wide = h.astype(F32)
    scale = lax.rsqrt(jnp.mean(wide**2, -1, keepdims=True) + 1e-6)
    return (wide * scale).astype(BF)


def tables(tokens):
    half = HEAD // 2
    angle = jnp.arange(tokens, dtype=F32)[:, None] * THETA ** (-jnp.arange(half, dtype=F32) / half)
    cos, sin = jnp.cos(angle), jnp.sin(angle)
    return jnp.concatenate([cos, cos], -1), jnp.concatenate([-sin, sin], -1)


def layer(h, w, whole, n, cos, sin):
    a = normed(h)
    q, k, v = (matmul(a, w[name]) for name in ("wq", "wk", "wv"))
    out, lse = attend(q, k, v, cos, sin)
    mid = h + matmul(out, w["wo"])
    b = normed(mid)
    gate, up, act = mlp(b, whole["w_gate"], whole["w_up"], n)
    return mid + matmul(act, w["w_down"]), (h, a, q, k, v, out, lse, mid, b, gate, up, act)


MLP, ATTENTION = ("w_gate", "w_up", "w_down"), ("wq", "wk", "wv", "wo")


def solution(mesh):
    tie = lax.optimization_barrier

    def scatter(g):
        return lax.psum_scatter(g, "dp", scatter_dimension=0, tiled=True)

    def gather(g):
        return lax.all_gather(g, "dp", axis=0, tiled=True)

    def step(x, dy, *arrays):
        weights, m, v = (dict(zip(NAMES, arrays[i : i + 7], strict=True)) for i in (0, 7, 14))
        count = weights["wq"].shape[0]
        layers = [{name: w[n] for name, w in weights.items()} for n in range(count)]
        cos, sin = tables(x.shape[1])
        h, kept = x[0], []
        for n, w in enumerate(layers):
            h, some = layer(h, w, weights, n, cos, sin)
            kept.append(some)
        d = dy[0]
        width, ff = weights["wq"].shape[2], weights["w_gate"].shape[2]
        cut = 8 * HEAD
        shards, full, gs = {}, {}, {}

        def send(n, tag, g, places, into=None, at=0):
            shards[n, tag] = scatter(g)
            for name, wide in places:
                gs.setdefault((n, name), []).append(((n, into or tag), at, wide))
                at += wide

        for n in reversed(range(count)):
            h, a, q, k, values, out, lse, mid, b, gate, up, act = kept[n]
            last = n == count - 1
            d, g = tie((d, grads((d, act[None]))))
            send(n, "down", g, [("w_down", ff)], "mlp", 2 * ff)
            d_gu = mlp_inner_bwd(d, weights["w_down"], gate, up, n)
            if not last:
                d_gu, shards[n + 1, "attention"] = tie((d_gu, shards[n + 1, "attention"]))
                full[n + 1, "attention"] = gather(shards[n + 1, "attention"])
            d_gu, g = tie((d_gu, grads((b, d_gu))))
            send(n, "mlp", g, [("w_gate", ff), ("w_up", ff)])
            d_mid = back(d_gu, (weights["w_gate"], weights["w_up"]), n, mid, d, 1024)
            if not last:
                d_mid, shards[n, "down"] = tie((d_mid, shards[n, "down"]))
            args = (q, k, values, by_left(d_mid, layers[n]["wo"]), out, lse, cos, sin)
            if n > 0:
                d = attend_bwd(*args, first=0, groups=1)
                d, shards[n, "down"], shards[n, "mlp"] = tie((d, shards[n, "down"], shards[n, "mlp"]))
                d, joined = tie((d, jnp.concatenate([shards[n, "mlp"], shards[n, "down"]], 1)))
                full[n, "mlp"] = gather(joined)
                d = attend_bwd(*args, first=1, groups=2, before=d)
                d, g = tie((d, grads((a, d), (d_mid, out[None]))))
                send(n, "attention", g, [("wq", width), ("wk", width), ("wv", width), ("wo", width)])
                d = back(d, tuple(weights[name] for name in ("wq", "wk", "wv")), n, h, d_mid, 768)
                d, full[n, "mlp"] = tie((d, full[n, "mlp"]))
            else:
                d = attend_bwd(*args, first=0, groups=2, whole=False)
                args, g, full[n + 1, "attention"] = tie((args, grads((a, d), (d_mid, out[None])), full[n + 1, "attention"]))
                send(n, "early", g, [("wq", cut), ("wk", cut), ("wv", cut), ("wo", width)])
                d = attend_bwd(*args, first=2, groups=1, whole=False)
                d, shards[n, "mlp"] = tie((d, shards[n, "mlp"]))
                d, joined = tie((d, jnp.concatenate([shards[n, "mlp"], shards[n, "down"]], 1)))
                g, shards[n, "early"] = tie((grads((a, d)), shards[n, "early"]))
                send(n, "late", g, [("wq", width - cut), ("wk", width - cut), ("wv", width - cut)], "early", 3 * cut + width)
        shards = dict(zip(shards, tie(tuple(shards.values()))))
        factor = clip_factor(tuple(shards.values()), mesh.shape["dp"], sum(w.size for w in weights.values()))
        full[0, "mlp"] = gather(tie((joined, shards[0, "late"]))[0])
        full[0, "early"] = gather(jnp.concatenate([shards[0, "early"], shards[0, "late"]], 1))
        got = {MLP: None, ATTENTION: None}
        for n in reversed(range(count)):
            for part, blocks in ((MLP, (16, 1)), (ATTENTION, (4, 4))):
                state = [of[name] for name in part for of in (weights, m, v)]
                pieces = [[(full[key], at, wide) for key, at, wide in gs[n, name]] for name in part]
                got[part] = update(factor, pieces, state, n, got[part], blocks)
                factor, got[part] = tie((factor, got[part]))
        new = {name: got[part][3 * i : 3 * i + 3] for part in got for i, name in enumerate(part)}
        return tuple(new[name][which] for which in range(3) for name in NAMES)

    states, all_of = P(("rep", "dp"), None, None), P(None, None, None)
    return jax.shard_map(
        step,
        mesh=mesh,
        in_specs=(states, states) + (all_of,) * 21,
        out_specs=(P("rep", None, None),) * 21,
        check_vma=False,
    )
```
